16 devices in a mesh: dp: 1, tp: 16 (over x, y, z, core).
Axes of the slice: x: 2, y: 2, z: 2, core: 2. Of those that a mesh axis runs over, the one named last changes fastest.
Arguments:
- x: bfloat16 [2048, 16384], P('dp')
- gain: bfloat16 [16384], replicated
- wq: bfloat16 [16384, 16384], P(None, 'tp')
- wk: bfloat16 [16384, 16384], P(None, 'tp')
- wv: bfloat16 [16384, 16384], P(None, 'tp')
- wo: bfloat16 [16384, 16384], P('tp')
Outputs:
- output: bfloat16 [2048, 16384], P('dp')
All inputs are finite; a program needn't handle non-finite values.
Results may differ from the reference program's by a relative error of at most 0.012.
Values are sent between devices in bfloat16 or wider.
A program may use at most 2 GiB of HBM per device.

```python
import jax
import jax.numpy as jnp
from jax import lax

ROWS = 2048
D = 16384
HEADS = 128
KV_HEADS = 128
HEAD = 128
THETA = 10000


def setup_inputs(seed: int = 0, part: int = 0) -> dict:
    kx, kn, kq, kk, kv, ko = jax.random.split(jax.random.key(seed), 6)

    def weights(key, rows, columns):
        return jax.random.normal(key, (rows, columns), jnp.float32) * rows**-0.5

    drawn = {
        "x": jax.random.normal(jax.random.fold_in(kx, part), (ROWS, D), jnp.float32),
        "gain": 1 + 0.1 * jax.random.normal(kn, (D,), jnp.float32),
        "wq": 2 * weights(kq, D, HEADS * HEAD),
        "wk": 2 * weights(kk, D, KV_HEADS * HEAD),
        "wv": 4 * weights(kv, D, KV_HEADS * HEAD),
        "wo": weights(ko, HEADS * HEAD, D),
    }
    return {k: v.astype(jnp.bfloat16) for k, v in drawn.items()}


def normed(x, gain):
    wide = x.astype(jnp.float32)
    scale = lax.rsqrt(jnp.mean(wide * wide, -1, keepdims=True) + 1e-6)
    return (wide * scale * gain.astype(jnp.float32)).astype(jnp.bfloat16)


def turned(t, place, theta):
    half = t.shape[-1] // 2
    angle = place.astype(jnp.float32)[:, None] * theta ** (-jnp.arange(half, dtype=jnp.float32) / half)
    cos, sin = jnp.cos(angle)[:, None], jnp.sin(angle)[:, None]
    a, b = t[..., :half].astype(jnp.float32), t[..., half:].astype(jnp.float32)
    return jnp.concatenate([a * cos - b * sin, b * cos + a * sin], -1).astype(jnp.bfloat16)


def matmul(a, w):
    return jnp.dot(a, w, preferred_element_type=jnp.float32).astype(jnp.bfloat16)


def einsum(form, a, b):
    return jnp.einsum(form, a.astype(jnp.float32), b.astype(jnp.float32))


def attention(q, k, v):
    scores = einsum("tgsd,ugd->gstu", q, k) * q.shape[-1] ** -0.5
    token = jnp.arange(q.shape[0])
    scores = jnp.where(token[:, None] >= token, scores, -jnp.inf)
    weights = jax.nn.softmax(scores, -1).astype(jnp.bfloat16)
    return einsum("gstu,ugd->tgsd", weights, v).astype(jnp.bfloat16)


def reference(x, gain, wq, wk, wv, wo):
    a, place = normed(x, gain), jnp.arange(ROWS)
    q = turned(matmul(a, wq).reshape(ROWS, HEADS, HEAD), place, THETA).reshape(ROWS, KV_HEADS, -1, HEAD)
    k = turned(matmul(a, wk).reshape(ROWS, KV_HEADS, HEAD), place, THETA)
    v = matmul(a, wv).reshape(ROWS, KV_HEADS, HEAD)
    seen = attention(q, k, v).reshape(ROWS, HEADS * HEAD)
    return (x.astype(jnp.float32) + jnp.dot(seen, wo, preferred_element_type=jnp.float32)).astype(jnp.bfloat16)
```

```python
import functools
from typing import NamedTuple

import jax
import jax.numpy as jnp
import numpy as np
from jax import lax
from jax.experimental import pallas as pl
from jax.experimental.pallas import tpu as pltpu
from jax.sharding import PartitionSpec as P

HEAD = 128
THETA = 10000
EPS = 1e-6
NEG = -1e30
HIDDEN = 2 * NEG
LOG2E = 1.4426950408889634
ONES = 16
NK = 8
NW = 8
LAG = 3
TILES = 3 * NK + NW


class Sizes(NamedTuple):
    rows: int
    wide: int
    heads: int
    m: int = 256
    slots: int = 4

    @property
    def blocks(self):
        return self.rows // self.m

    @property
    def inner(self):
        return self.heads * HEAD

    @property
    def half(self):
        return self.wide // 2

    @property
    def kt(self):
        return self.wide // NK

    @property
    def wt(self):
        return self.half // NW

    @property
    def parts(self):
        u = self.wt // 2
        return (0, 6 * u), (6 * u, 5 * u), (11 * u, 5 * u)


QKV_ACTIONS = {
    0: ("gather2", 0, 2), 1: ("gather2", 1, 2), 2: ("gather2", 2, 2),
    3: ("last", 0, 3), 4: ("last", 1, 3), 5: ("last", 2, 3),
    9: ("add1", 0, 1), 10: ("add1", 1, 1), 11: ("add1", 2, 1),
    15: ("gather3", 0, 2), 16: ("gather3", 1, 2), 17: ("gather3", 2, 2),
    20: ("add2", 0, 1), 21: ("add2", 1, 1), 22: ("add2", 2, 1),
}
WO_ACTIONS = {2: 0, 5: 1, 7: 2}


def _dot(a, b, ca, cb):
    return lax.dot_general(a, b, (((ca,), (cb,)), ((), ())), preferred_element_type=jnp.float32)


def _kernel(sz, x, wq, wk, wv, wo, gain, table, y, wpart,
            a, wb, kc, vt, q, seen, seenp, acc, mix, top, keep, send1, recv1, send2, recv2, send3, recv3, fin, xr,
            w_sem, x_sem, xr_sem, wx_sem, seen_send, seen_recv, s_sem, r_sem, g_send, g_recv, own_sem, d_send, d_recv):
    m, nb, heads, inner, half, kt, wt = sz.m, sz.blocks, sz.heads, sz.inner, sz.half, sz.kt, sz.wt
    total = nb * TILES
    me = lax.axis_index("tp")
    core = lax.rem(me, 2)
    mate = me + 1 - 2 * core
    mine, other = pl.multiple_of(core * half, 128), pl.multiple_of((1 - core) * half, 128)

    def local(src, dst, sem):
        return pltpu.make_async_copy(src, dst, sem)

    def remote(src, dst, send, recv, to):
        return pltpu.make_async_remote_copy(src_ref=src, dst_ref=dst, send_sem=send, recv_sem=recv, device_id={"tp": to},
                                            device_id_type=pl.DeviceIdType.MESH)

    def rows_of(i, n):
        return pl.ds(pl.multiple_of(i, 16), n)


    def x_copy(b, k):
        return local(x.at[rows_of(b * m, m), pl.ds(k * kt, kt)], a.at[k], x_sem.at[k])

    wx = remote(wo.at[:, pl.ds(other, half)], wpart, wx_sem.at[0], wx_sem.at[1], mate)

    def fetch(g):
        s, j = lax.rem(g, sz.slots), lax.rem(g, TILES)
        which, first = lax.div(j, NK), pl.multiple_of(lax.rem(j, NK) * kt, 16)
        for i, w in enumerate((wq, wk, wv)):
            @pl.when(which == i)
            def _():
                local(w.at[pl.ds(first, kt)], wb.at[s], w_sem.at[s, 0]).start()

        @pl.when(g == 3 * NK)
        def _():
            wx.wait_recv()

        @pl.when(which >= 3)
        def _():
            c = pl.multiple_of((j - 3 * NK) * wt, 128)
            local(wo.at[:, pl.ds(pl.multiple_of(mine + c, 128), wt)], wb.at[s, pl.ds(0, inner), pl.ds(0, wt)], w_sem.at[s, 0]).start()
            local(wpart.at[:, pl.ds(c, wt)], wb.at[s, pl.ds(inner, inner), pl.ds(0, wt)], w_sem.at[s, 1]).start()

    def next_tile(g):
        @pl.when(g + sz.slots - 1 < total)
        def _():
            fetch(g + sz.slots - 1)


    def way(p, b, stage):
        axis = lax.rem(p + stage + b, 3)
        mask = 8 - 5 * axis + axis * axis
        bit = lax.rem(lax.div(me, mask), 2)
        return bit, me + mask * (1 - 2 * bit)

    def ways(p, b):
        return [way(p, b, stage) for stage in range(3)]

    def place(p, b, off, n):
        return rows_of(b * m + off, n), pl.ds(pl.multiple_of(mine + sz.parts[p][0], 128), sz.parts[p][1])

    def cols(p):
        return pl.ds(*sz.parts[p])

    def strips(p, body):
        c0, n = sz.parts[p]
        step = sz.wt // 2

        def one(i, _):
            body(pl.ds(pl.multiple_of(c0 + i * step, 128), step))
            return 0

        lax.fori_loop(0, n // step, one, 0)

    def wide(v):
        return v.astype(jnp.float32)

    def stage1(p, b):
        return remote(send1.at[:, cols(p)], recv1.at[lax.rem(b, 2), :, cols(p)], s_sem.at[0, p], r_sem.at[0, lax.rem(b, 2), p],
                      ways(p, b)[0][1])

    def stage2(p, b):
        return remote(send2.at[:, cols(p)], recv2.at[lax.rem(b, 2), :, cols(p)], s_sem.at[1, p], r_sem.at[1, lax.rem(b, 2), p],
                      ways(p, b)[1][1])

    def stage3(p, b):
        return remote(send3.at[:, cols(p)], recv3.at[lax.rem(b, 2), :, cols(p)], s_sem.at[2, p], r_sem.at[2, lax.rem(b, 2), p],
                      ways(p, b)[2][1])

    def offsets(p, b):
        (b1, _), (b2, _), (b3, _) = ways(p, b)
        return b1 * (m // 2), b1 * (m // 2) + b2 * (m // 4), b1 * (m // 2) + b2 * (m // 4) + b3 * (m // 8)

    def xr_copy(p, b):
        return local(x.at[place(p, b, offsets(p, b)[2], m // 8)], xr.at[:, cols(p)], xr_sem.at[p])

    def own_copy(p, b):
        return local(fin.at[:, cols(p)], y.at[place(p, b, offsets(p, b)[2], m // 8)], own_sem.at[p])

    def gather(stage, p, b):
        w = ways(p, b)
        n = m // 8 << stage
        at = place(p, b, offsets(p, b)[2 - stage], n)
        src = fin.at[:, cols(p)] if stage == 0 else y.at[at]
        return remote(src, y.at[at], g_send.at[stage, p], g_recv.at[stage, lax.rem(b, 2), p], w[2 - stage][1])

    def pass_on(kind, p, b):
        o = offsets(p, b)
        w = ways(p, b)
        if kind == 0:
            at, src = place(p, b, o[2], m // 8), fin.at[:, cols(p)]
        else:
            n = m // 8 << (kind - 1)
            base = (o[1], o[0], 0)[kind - 1]
            at = place(p, b, base + (1 - w[3 - kind][0]) * n, n)
            src = y.at[at]
        return remote(src, y.at[at], d_send.at[kind, p], d_recv.at[b], mate)

    def add1(p, b):
        s, w = lax.rem(b, 2), ways(p, b)
        stage1(p, b).wait()
        h = m // 4
        go, stay = rows_of((1 - w[1][0]) * h, h), rows_of(w[1][0] * h, h)

        def body(c):
            send2[:, c] = (keep[go, c] + wide(recv1[s, go, c])).astype(send2.dtype)
            keep[stay, c] = keep[stay, c] + wide(recv1[s, stay, c])

        strips(p, body)
        stage2(p, b).start()

    def add2(p, b):
        s, w = lax.rem(b, 2), ways(p, b)
        xr_copy(p, b).start()
        stage2(p, b).wait()
        h = m // 8
        base, go, stay = w[1][0] * (m // 4), (1 - w[2][0]) * h, w[2][0] * h

        def body(c):
            send3[:, c] = (keep[rows_of(base + go, h), c] + wide(recv2[s, rows_of(go, h), c])).astype(send3.dtype)
            keep[rows_of(base + stay, h), c] = keep[rows_of(base + stay, h), c] + wide(recv2[s, rows_of(stay, h), c])

        strips(p, body)
        stage3(p, b).start()

    def add3(p, b):
        s, w = lax.rem(b, 2), ways(p, b)
        xr_copy(p, b).wait()
        stage3(p, b).wait()
        h = m // 8
        at = rows_of(w[1][0] * (m // 4) + w[2][0] * h, h)

        def body(c):
            fin[:, c] = (wide(xr[:, c]) + (keep[at, c] + wide(recv3[s, :, c]))).astype(fin.dtype)

        strips(p, body)
        gather(0, p, b).start()
        own_copy(p, b).start()
        pass_on(0, p, b).start()

    def gather2(p, b):
        own_copy(p, b).wait()
        gather(0, p, b).wait()
        gather(1, p, b).start()
        pass_on(1, p, b).start()
        pass_on(0, p, b).wait_send()

    def gather3(p, b):
        gather(1, p, b).wait()
        gather(2, p, b).start()
        pass_on(2, p, b).start()
        pass_on(1, p, b).wait_send()

    def last(p, b):
        gather(2, p, b).wait()
        pass_on(2, p, b).wait_send()

        @pl.when(b > 0)
        def _():
            pass_on(3, p, b - 1).wait_send()

        pass_on(3, p, b).start()

    stages = {"add1": add1, "add2": add2, "add3": add3, "gather2": gather2, "gather3": gather3, "last": last}

    def act(stage, p, b):
        @pl.when((b >= 0) & (b < nb))
        def _():
            stages[stage](p, b)


    def norm():
        group = 32

        def one(i, _):
            at = pl.ds(pl.multiple_of(i * group, group), group)
            total = jnp.zeros((group, 128), jnp.float32)
            for k in range(NK):
                v = wide(a[k, at, :])
                v = v * v
                for c in range(0, kt, 128):
                    total = total + v[:, c : c + 128]
            scale = lax.rsqrt(jnp.sum(total, axis=1, keepdims=True) * (1 / sz.wide) + EPS)
            for k in range(NK):
                a[k, at, :] = (wide(a[k, at, :]) * scale * gain[k]).astype(a.dtype)
            return 0

        lax.fori_loop(0, m // group, one, 0)

    def turn(b, put):
        t = table[rows_of(b * m, m), :]
        r = pltpu.roll(t, HEAD // 2, 1)
        low = lax.broadcasted_iota(jnp.int32, t.shape, 1) < HEAD // 2
        cos, sin = jnp.where(low, t, r), jnp.where(low, -r, t)
        for h in range(heads):
            v = wide(acc[:, h * HEAD : (h + 1) * HEAD].astype(q.dtype))
            put(h, (v * cos + pltpu.roll(v, HEAD // 2, 1) * sin).astype(q.dtype))

    def put_q(b):
        def put(h, v):
            q[h] = v
        turn(b, put)

    def put_k(b):
        def put(h, v):
            kc[h, rows_of(b * m, m), :] = v
        turn(b, put)

    def put_v(b):
        for h in range(heads):
            vt[h, 0:HEAD, pl.ds(pl.multiple_of(b * m, 128), m)] = acc[:, h * HEAD : (h + 1) * HEAD].T.astype(vt.dtype)

    def attention(b):
        e = HEAD**-0.5 * LOG2E
        top[...] = jnp.full(top.shape, NEG, jnp.float32)
        mix[...] = jnp.zeros(mix.shape, jnp.float32)
        group = min(heads, 4)

        def keys(j, masked):
            at = pl.multiple_of(j * m, m)
            for h0 in range(0, heads, group):
                hs = range(h0, h0 + group)
                scores = [_dot(kc[h, pl.ds(at, m), :], q[h], 1, 1) for h in hs]
                weights, keeps = [], []
                for h, s in zip(hs, scores):
                    if masked:
                        ok = lax.broadcasted_iota(jnp.int32, s.shape, 0) <= lax.broadcasted_iota(jnp.int32, s.shape, 1)
                        s = jnp.where(ok, s, HIDDEN)
                    old = top[h : h + 1, :]
                    new = jnp.maximum(old, s.max(axis=0, keepdims=True))
                    top[h : h + 1, :] = new
                    weights.append(jnp.exp2((s - new) * e).astype(vt.dtype))
                    keeps.append(jnp.exp2((old - new) * e))
                for h, w, k in zip(hs, weights, keeps):
                    mix[h] = mix[h] * k + _dot(vt[h, :, pl.ds(at, m)], w, 1, 0)

        def whole(j, _):
            keys(j, False)
            return 0

        lax.fori_loop(0, b, whole, 0)
        keys(b, True)
        for h in range(heads):
            got = mix[h, 0:HEAD, :] * (1 / mix[h, HEAD : HEAD + 1, :])
            seen[:, h * HEAD : (h + 1) * HEAD] = got.T.astype(seen.dtype)

    def seen_copy(b):
        s = lax.rem(b, 2)
        return remote(seen, seenp.at[s], seen_send, seen_recv.at[s], mate)


    for k in range(NK):
        x_copy(0, k).start()
    for g in range(sz.slots - 1):
        fetch(jnp.int32(g))
    barrier = pltpu.get_barrier_semaphore()
    friends = [mate] + [way(0, 0, stage)[1] for stage in range(3)]
    for friend in friends:
        pl.semaphore_signal(barrier, inc=1, device_id={"tp": friend}, device_id_type=pl.DeviceIdType.MESH)
    pl.semaphore_wait(barrier, len(friends))
    wx.start()
    for h in range(heads):
        vt[h, HEAD:, :] = jnp.ones((ONES, sz.rows), vt.dtype)

    def block(b, _):
        live = b < nb

        @pl.when(live)
        def _():
            for k in range(NK):
                x_copy(b, k).wait()
            norm()

        def qkv_tick(t, _):
            @pl.when(live)
            def _():
                g = b * TILES + t
                s, k = lax.rem(g, sz.slots), lax.rem(t, NK)
                next_tile(g)
                local(wq.at[pl.ds(0, kt)], wb.at[s], w_sem.at[s, 0]).wait()

                @pl.when(k == 0)
                def _():
                    acc[...] = jnp.zeros(acc.shape, jnp.float32)

                acc[...] += jnp.dot(a[k], wb[s], preferred_element_type=jnp.float32)
                for i, put in enumerate((put_q, put_k, put_v)):
                    @pl.when(t == NK * (i + 1) - 1)
                    def _():
                        put(b)

            for at, (stage, p, back) in QKV_ACTIONS.items():
                @pl.when(t == at)
                def _():
                    act(stage, p, b - back)
            return 0

        lax.fori_loop(0, 3 * NK, qkv_tick, 0)

        @pl.when(live)
        def _():
            @pl.when(b + 1 < nb)
            def _():
                for k in range(NK):
                    x_copy(b + 1, k).start()

            @pl.when(b > 0)
            def _():
                seen_copy(b - 1).wait_send()

            attention(b)
            seen_copy(b).start()

        for p in range(3):
            act("add3", p, b - 1)

        @pl.when(live)
        def _():
            seen_copy(b).wait_recv()

        def wo_tick(t, _):
            @pl.when(live)
            def _():
                g = b * TILES + 3 * NK + t
                s = lax.rem(g, sz.slots)
                next_tile(g)
                for i in range(2):
                    local(wo.at[:, pl.ds(0, wt)], wb.at[s, pl.ds(i * inner, inner), pl.ds(0, wt)], w_sem.at[s, i]).wait()
                for j in range(2):
                    n = t * 2 + j
                    p = jnp.where(n < 6, 0, jnp.where(n < 11, 1, 2))
                    bit = way(p, b, 0)[0]
                    go, stay = rows_of((1 - bit) * (m // 2), m // 2), rows_of(bit * (m // 2), m // 2)
                    ps = lax.rem(b, 2)
                    here = jnp.concatenate([seen[go, :], seen[stay, :]], axis=0)
                    there = jnp.concatenate([seenp[ps, go, :], seenp[ps, stay, :]], axis=0)
                    c = slice(j * (wt // 2), (j + 1) * (wt // 2))
                    r = jnp.dot(here, wb[s, 0:inner, c], preferred_element_type=jnp.float32)
                    r = r + jnp.dot(there, wb[s, inner : 2 * inner, c], preferred_element_type=jnp.float32)
                    out = pl.ds(pl.multiple_of(n * (wt // 2), 128), wt // 2)
                    send1[:, out] = r[: m // 2].astype(send1.dtype)
                    keep[:, out] = r[m // 2 :]
                for at, p in WO_ACTIONS.items():
                    @pl.when(t == at)
                    def _():
                        stage1(p, b).start()
            return 0

        lax.fori_loop(0, NW, wo_tick, 0)
        return 0

    lax.fori_loop(0, nb + LAG, block, 0)
    seen_copy(jnp.int32(nb - 1)).wait_send()
    wx.wait_send()
    for p in range(3):
        pass_on(3, p, jnp.int32(nb - 1)).wait_send()
    for b in range(nb):
        rest = y.at[pl.ds(b * m, m), pl.ds(other, half)]
        remote(rest, rest, d_send.at[0, 0], d_recv.at[b], mate).wait_recv()


def _angles(rows):
    half = HEAD // 2
    step = np.power(np.float32(THETA), -np.arange(half, dtype=np.float32) / np.float32(half)).astype(np.float32)
    angle = (np.arange(rows, dtype=np.float32)[:, None] * step).astype(np.float64)
    return np.concatenate([np.cos(angle), np.sin(angle)], -1).astype(np.float32)


def layer(sz, x, gain, wq, wk, wv, wo):
    low, f32 = x.dtype, jnp.float32
    m, inner, half = sz.m, sz.inner, sz.half
    vmem, dma = pltpu.VMEM, pltpu.SemaphoreType.DMA
    scratch = [
        vmem((NK, m, sz.kt), low),
        vmem((sz.slots, max(sz.kt, 2 * inner), max(inner, sz.wt)), low),
        vmem((sz.heads, sz.rows, HEAD), low),
        vmem((sz.heads, HEAD + ONES, sz.rows), low),
        vmem((sz.heads, m, HEAD), low),
        vmem((m, inner), low),
        vmem((2, m, inner), low),
        vmem((m, inner), f32),
        vmem((sz.heads, HEAD + ONES, m), f32),
        vmem((sz.heads, m), f32),
        vmem((m // 2, half), f32),
        vmem((m // 2, half), low),
        vmem((2, m // 2, half), low),
        vmem((m // 4, half), low),
        vmem((2, m // 4, half), low),
        vmem((m // 8, half), low),
        vmem((2, m // 8, half), low),
        vmem((m // 8, half), low),
        vmem((m // 8, half), low),
        dma((sz.slots, 2)), dma((NK,)), dma((3,)), dma((2,)), dma, dma((2,)),
        dma((3, 3)), dma((3, 2, 3)), dma((3, 3)), dma((3, 2, 3)), dma((3,)), dma((4, 3)), dma((sz.blocks,)),
    ]
    hbm, here = pl.BlockSpec(memory_space=pl.ANY), pl.BlockSpec(memory_space=pltpu.VMEM)
    flops = 2 * sz.rows * sz.wide * 4 * inner + 2 * sz.rows * sz.rows * 2 * inner
    y, _ = pl.pallas_call(
        functools.partial(_kernel, sz),
        out_shape=[jax.ShapeDtypeStruct(x.shape, low), jax.ShapeDtypeStruct((inner, half), low)],
        in_specs=[hbm] * 5 + [here] * 2,
        out_specs=[hbm, hbm],
        scratch_shapes=scratch,
        compiler_params=pltpu.CompilerParams(collective_id=0, has_side_effects=True, vmem_limit_bytes=67043328),
        cost_estimate=pl.CostEstimate(flops=flops, bytes_accessed=4 * sz.blocks * inner * sz.wide * 2,
                                      transcendentals=sz.rows * sz.rows * sz.heads),
        name="decoder_attention",
    )(x, wq, wk, wv, wo, gain.astype(f32).reshape(NK, 1, sz.kt), jnp.asarray(_angles(sz.rows)))
    return y


def solution(mesh):
    def step(x, gain, wq, wk, wv, wo):
        sz = Sizes(rows=x.shape[0], wide=x.shape[1], heads=wq.shape[1] // HEAD)
        return layer(sz, x, gain, wq, wk, wv, wo)

    tokens, columns = P("dp", None), P(None, "tp")
    return jax.shard_map(
        step,
        mesh=mesh,
        in_specs=(tokens, P(None), columns, columns, columns, P("tp", None)),
        out_specs=tokens,
        check_vma=False,
    )
```

```python
import functools
from typing import NamedTuple

import jax
import jax.numpy as jnp
import numpy as np
from jax import lax
from jax.experimental import pallas as pl
from jax.experimental.pallas import tpu as pltpu
from jax.sharding import PartitionSpec as P

HEAD = 128
THETA = 10000
EPS = 1e-6
NEG = -1e30
HIDDEN = 2 * NEG
LOG2E = 1.4426950408889634
ONES = 16
NK = 8
NW = 8
TILES = 3 * NK + NW
MID = 3 * NK
STEPS = MID + 1 + NW


class Sizes(NamedTuple):
    rows: int
    wide: int
    heads: int
    m: int = 256
    slots: int = 5

    @property
    def blocks(self):
        return self.rows // self.m

    @property
    def inner(self):
        return self.heads * HEAD

    @property
    def half(self):
        return self.wide // 2

    @property
    def kt(self):
        return self.wide // NK

    @property
    def wt(self):
        return self.half // NW

    @property
    def parts(self):
        u = self.wt // 2
        return (0, 6 * u), (6 * u, 5 * u), (11 * u, 5 * u)


WHEN = {
    "add1": (10, 9, 11),
    "add2": (18, 15, 19),
    "add3": (24, 21, 23),
    "gather2": (30, 38, 27),
    "gather3": (47, 48, 43),
    "last": (76, 73, 63),
}
SENT = {MID + 3: 0, MID + 6: 1, MID + 8: 2}
LAG = max(max(w) for w in WHEN.values()) // STEPS + 1


def _agenda(step):
    return [(stage, p, 1 + w[p] // STEPS) for stage, w in WHEN.items() for p in range(3) if w[p] % STEPS == step]


def _dot(a, b, ca, cb):
    return lax.dot_general(a, b, (((ca,), (cb,)), ((), ())), preferred_element_type=jnp.float32)


def _kernel(sz, x, wq, wk, wv, wo, angles, gain, y, wpart,
            a, xb, ssq, wb, table, kc, vt, q, seen, seenp, acc, mix, top, keep, send1, recv1, send2, recv2, send3, recv3, fin, xr,
            w_sem, x_sem, n_send, n_recv, t_sem, xr_sem, wx_sem, seen_send, seen_recv, s_sem, r_sem, g_send, g_recv, own_sem, d_send, d_recv):
    m, nb, heads, inner, half, kt, wt = sz.m, sz.blocks, sz.heads, sz.inner, sz.half, sz.kt, sz.wt
    total = nb * TILES
    me = lax.axis_index("tp")
    core = lax.rem(me, 2)
    mate = me + 1 - 2 * core
    mine, other = pl.multiple_of(core * half, 128), pl.multiple_of((1 - core) * half, 128)

    def local(src, dst, sem):
        return pltpu.make_async_copy(src, dst, sem)

    def remote(src, dst, send, recv, to):
        return pltpu.make_async_remote_copy(src_ref=src, dst_ref=dst, send_sem=send, recv_sem=recv, device_id={"tp": to},
                                            device_id_type=pl.DeviceIdType.MESH)

    def rows_of(i, n):
        return pl.ds(pl.multiple_of(i, 16), n)


    def x_copy(b, k):
        at = rows_of(b * m + core * (m // 2), m // 2)
        return local(x.at[at, pl.ds(pl.multiple_of(k * kt, 128), kt)], xb.at[k], x_sem.at[k])

    def share(k):
        part = a.at[k, rows_of(core * (m // 2), m // 2)]
        return remote(part, part, n_send.at[k], n_recv.at[k], mate)

    wx = remote(wo.at[:, pl.ds(other, half)], wpart, wx_sem.at[0], wx_sem.at[1], mate)

    def fetch(g, j):
        s = lax.rem(g, sz.slots)

        def weight(w, k):
            local(w.at[rows_of(k * kt, kt)], wb.at[s], w_sem.at[s, 0]).start()

        def out(t):
            c = pl.multiple_of(t * wt, 128)
            local(wo.at[:, pl.ds(pl.multiple_of(mine + c, 128), wt)], wb.at[s, pl.ds(0, inner), pl.ds(0, wt)], w_sem.at[s, 0]).start()
            local(wpart.at[:, pl.ds(c, wt)], wb.at[s, pl.ds(inner, inner), pl.ds(0, wt)], w_sem.at[s, 1]).start()

        for i, w in enumerate((wq, wk, wv)):
            yield lambda w=w, i=i: weight(w, j - i * NK)
        yield lambda: out(j - 3 * NK)

    ahead = sz.slots - 1

    def next_tile(g, phase, step):
        last = (phase + 1) * NK - ahead
        here, there = list(fetch(g + ahead, step + ahead)), list(fetch(g + ahead, step + ahead - (TILES if phase == 3 else 0)))

        @pl.when(step < last)
        def _():
            here[phase]()

        @pl.when((step >= last) & (g + ahead < total))
        def _():
            if phase == 2:
                @pl.when(g == 3 * NK - ahead)
                def _():
                    wx.wait_recv()

            there[(phase + 1) % 4]()

    def table_copy(b):
        return local(angles.at[rows_of(b * m, m)], table, t_sem)


    def way(p, b, stage):
        axis = lax.rem(p + stage + b, 3)
        mask = 8 - 5 * axis + axis * axis
        bit = lax.rem(lax.div(me, mask), 2)
        return bit, me + mask * (1 - 2 * bit)

    def ways(p, b):
        return [way(p, b, stage) for stage in range(3)]

    def place(p, b, off, n):
        return rows_of(b * m + off, n), pl.ds(pl.multiple_of(mine + sz.parts[p][0], 128), sz.parts[p][1])

    def cols(p):
        return pl.ds(*sz.parts[p])

    def strips(p, body):
        c0, n = sz.parts[p]
        step = sz.wt // 2

        def one(i, _):
            body(pl.ds(pl.multiple_of(c0 + i * step, 128), step))
            return 0

        lax.fori_loop(0, n // step, one, 0)

    def wide(v):
        return v.astype(jnp.float32)

    def stage1(p, b):
        return remote(send1.at[:, cols(p)], recv1.at[:, cols(p)], s_sem.at[0, p], r_sem.at[0, lax.rem(b, 2), p],
                      ways(p, b)[0][1])

    def stage2(p, b):
        return remote(send2.at[:, cols(p)], recv2.at[:, cols(p)], s_sem.at[1, p], r_sem.at[1, lax.rem(b, 2), p],
                      ways(p, b)[1][1])

    def stage3(p, b):
        return remote(send3.at[:, cols(p)], recv3.at[lax.rem(b, 2), :, cols(p)], s_sem.at[2, p], r_sem.at[2, lax.rem(b, 2), p],
                      ways(p, b)[2][1])

    def offsets(p, b):
        (b1, _), (b2, _), (b3, _) = ways(p, b)
        return b1 * (m // 2), b1 * (m // 2) + b2 * (m // 4), b1 * (m // 2) + b2 * (m // 4) + b3 * (m // 8)

    def xr_copy(p, b):
        return local(x.at[place(p, b, offsets(p, b)[2], m // 8)], xr.at[:, cols(p)], xr_sem.at[p])

    def own_copy(p, b):
        return local(fin.at[:, cols(p)], y.at[place(p, b, offsets(p, b)[2], m // 8)], own_sem.at[p])

    def gather(kind, p, b):
        w, o = ways(p, b), offsets(p, b)
        n, axis = m // 8, (2, 1, 0, 1, 0, 0)[kind]
        if kind < 3:
            at, src = place(p, b, o[2], n), fin.at[:, cols(p)]
        else:
            if kind < 5:
                at = place(p, b, o[1] + (1 - w[2][0]) * n, n)
            else:
                at = place(p, b, o[0] + (1 - w[1][0]) * 2 * n, 2 * n)
            src = y.at[at]
        return remote(src, y.at[at], g_send.at[kind, p], g_recv.at[kind, lax.rem(b, 2), p], w[axis][1])

    def pass_on(kind, p, b):
        o = offsets(p, b)
        w = ways(p, b)
        if kind == 0:
            at, src = place(p, b, o[2], m // 8), fin.at[:, cols(p)]
        else:
            n = m // 8 << (kind - 1)
            base = (o[1], o[0], 0)[kind - 1]
            at = place(p, b, base + (1 - w[3 - kind][0]) * n, n)
            src = y.at[at]
        return remote(src, y.at[at], d_send.at[kind, p], d_recv.at[b], mate)

    def add1(p, b):
        w = ways(p, b)
        stage1(p, b).wait()
        h = m // 4
        go, stay = rows_of((1 - w[1][0]) * h, h), rows_of(w[1][0] * h, h)

        def body(c):
            send2[:, c] = (keep[go, c] + wide(recv1[go, c])).astype(send2.dtype)
            keep[stay, c] = keep[stay, c] + wide(recv1[stay, c])

        strips(p, body)
        stage2(p, b).start()

    def add2(p, b):
        w = ways(p, b)
        xr_copy(p, b).start()
        stage2(p, b).wait()
        h = m // 8
        base, go, stay = w[1][0] * (m // 4), (1 - w[2][0]) * h, w[2][0] * h

        def body(c):
            send3[:, c] = (keep[rows_of(base + go, h), c] + wide(recv2[rows_of(go, h), c])).astype(send3.dtype)
            keep[rows_of(base + stay, h), c] = keep[rows_of(base + stay, h), c] + wide(recv2[rows_of(stay, h), c])

        strips(p, body)
        stage3(p, b).start()

    def fin_sent(p, b):
        for kind in range(3):
            gather(kind, p, b).wait_send()
        own_copy(p, b).wait()
        pass_on(0, p, b).wait_send()

    def add3(p, b):
        s, w = lax.rem(b, 2), ways(p, b)

        @pl.when(b > 0)
        def _():
            fin_sent(p, b - 1)

        xr_copy(p, b).wait()
        stage3(p, b).wait()
        h = m // 8
        at = rows_of(w[1][0] * (m // 4) + w[2][0] * h, h)

        def body(c):
            fin[:, c] = (wide(xr[:, c]) + (keep[at, c] + wide(recv3[s, :, c]))).astype(fin.dtype)

        strips(p, body)
        for kind in range(3):
            gather(kind, p, b).start()
        own_copy(p, b).start()
        pass_on(0, p, b).start()

    def gather2(p, b):
        gather(0, p, b).wait_recv()
        for kind in (3, 4):
            gather(kind, p, b).start()
        pass_on(1, p, b).start()

    def gather3(p, b):
        gather(1, p, b).wait_recv()
        gather(3, p, b).wait_recv()
        gather(5, p, b).start()
        pass_on(2, p, b).start()
        gather(3, p, b).wait_send()
        pass_on(1, p, b).wait_send()

    def last(p, b):
        for kind in (2, 4, 5):
            gather(kind, p, b).wait_recv()
        for kind in (4, 5):
            gather(kind, p, b).wait_send()
        pass_on(2, p, b).wait_send()

        @pl.when(b > 0)
        def _():
            pass_on(3, p, b - 1).wait_send()

        pass_on(3, p, b).start()

    stages = {"add1": add1, "add2": add2, "add3": add3, "gather2": gather2, "gather3": gather3, "last": last}

    def act(stage, p, b):
        @pl.when((b >= 0) & (b < nb))
        def _():
            stages[stage](p, b)


    def survey(b):
        ssq[...] = jnp.zeros(ssq.shape, jnp.float32)

        def one(k, _):
            x_copy(b, k).wait()
            total = ssq[...]
            for c in range(0, kt, 128):
                v = wide(xb[k, :, c : c + 128])
                total = total + v * v
            ssq[...] = total
            return 0

        lax.fori_loop(0, NK, one, 0)
        total = jnp.sum(ssq[...], axis=1, keepdims=True)
        ssq[...] = jnp.broadcast_to(lax.rsqrt(total * (1 / sz.wide) + EPS), ssq.shape)

    def normed(k, first, n):
        at, to = slice(first, first + n), rows_of(core * (m // 2) + first, n)
        for c in range(0, kt, 128):
            v = wide(xb[k, at, c : c + 128]) * ssq[at, :] * gain[k, :, c : c + 128]
            a[k, to, c : c + 128] = v.astype(a.dtype)

    def turn(b, put):
        t = table[...]
        r = pltpu.roll(t, HEAD // 2, 1)
        low = lax.broadcasted_iota(jnp.int32, t.shape, 1) < HEAD // 2
        cos, sin = jnp.where(low, t, r), jnp.where(low, -r, t)
        for h in range(heads):
            v = wide(acc[:, h * HEAD : (h + 1) * HEAD].astype(q.dtype))
            put(h, (v * cos + pltpu.roll(v, HEAD // 2, 1) * sin).astype(q.dtype))

    def put_q(b):
        def put(h, v):
            q[h] = v
        turn(b, put)

    def put_k(b):
        def put(h, v):
            kc[h, rows_of(b * m, m), :] = v
        turn(b, put)

    def put_v(b):
        for h in range(heads):
            vt[h, 0:HEAD, pl.ds(pl.multiple_of(b * m, 128), m)] = acc[:, h * HEAD : (h + 1) * HEAD].T.astype(vt.dtype)

    e = HEAD**-0.5 * LOG2E
    group = min(heads, 4)

    def own(j):
        return pl.ds(pl.multiple_of(j * m, m), m)

    def score(j, h):
        return _dot(kc[h, own(j), :], q[h], 1, 1)

    def weigh(h, s, masked):
        if masked:
            ok = lax.broadcasted_iota(jnp.int32, s.shape, 0) <= lax.broadcasted_iota(jnp.int32, s.shape, 1)
            s = jnp.where(ok, s, HIDDEN)
        old = top[h]
        new = jnp.maximum(old, s.max(axis=0, keepdims=True))
        top[h] = new
        return jnp.exp2((s - new) * e).astype(vt.dtype), jnp.exp2((old - new) * e)

    def blend(j, h, w, k):
        mix[h] = mix[h] * k + _dot(vt[h, :, own(j)], w, 1, 0)

    def attend(j, hs, masked, pieces):
        n, r = len(pieces), len(hs)
        s, w = {}, {}

        def share(i):
            return range(r * i // n, r * (i + 1) // n) if 0 <= i < n else ()

        for i in range(n + 2):
            for h in share(i - 1):
                w[h] = weigh(hs[h], s.pop(h), masked)
            for h in share(i):
                s[h] = score(j, hs[h])
            for h in share(i - 2):
                blend(j, hs[h], *w.pop(h))
            if i < n:
                pieces[i]()

    def forget():
        top[...] = jnp.full(top.shape, NEG, jnp.float32)
        mix[...] = jnp.zeros(mix.shape, jnp.float32)

    def attention(b):
        attend(b, range(heads), True, [lambda: None] * 2)
        for h in range(heads):
            got = mix[h, 0:HEAD, :] * (1 / mix[h, HEAD : HEAD + 1, :])
            seen[:, h * HEAD : (h + 1) * HEAD] = got.T.astype(seen.dtype)

    def seen_copy(b):
        s = lax.rem(b, 2)
        return remote(seen, seenp.at[s], seen_send, seen_recv.at[s], mate)


    for k in range(NK):
        x_copy(0, k).start()
    for g in range(ahead):
        list(fetch(jnp.int32(g), g))[0]()
    table_copy(0).start()
    barrier = pltpu.get_barrier_semaphore()
    friends = [mate] + [way(0, 0, stage)[1] for stage in range(3)]
    for friend in friends:
        pl.semaphore_signal(barrier, inc=1, device_id={"tp": friend}, device_id_type=pl.DeviceIdType.MESH)

    survey(0)
    pl.semaphore_wait(barrier, len(friends))
    forget()

    def first(k, _):
        normed(k, 0, m // 2)
        share(k).start()
        x_copy(1, k).start()
        return 0

    lax.fori_loop(0, NK, first, 0)
    wx.start()
    for h in range(heads):
        vt[h, HEAD:, :] = jnp.ones((ONES, sz.rows), vt.dtype)

    def block(b, _):
        live = b < nb

        @pl.when(live)
        def _():
            table_copy(b).wait()

        def actions(step, steps):
            for at in steps:
                for stage, p, back in _agenda(at):
                    @pl.when(step == at)
                    def _():
                        act(stage, p, b - back)

        def tick(phase, step):
            g = b * TILES + step
            s, k = lax.rem(g, sz.slots), lax.rem(step, NK)
            next_tile(g, phase, step)
            if phase == 0:
                share(k).wait()
            local(wq.at[pl.ds(0, kt)], wb.at[s], w_sem.at[s, 0]).wait()

            n = 4

            def piece(i):
                c = slice(i * inner // n, (i + 1) * inner // n)
                acc[:, c] += jnp.dot(a[k], wb[s, :, c], preferred_element_type=jnp.float32)

            pieces = [functools.partial(piece, i) for i in range(n)]

            def plain():
                for one in pieces:
                    one()

            if phase == 0:
                plain()
            else:
                i = (step - NK) * group
                j, h0 = lax.div(i, heads), lax.rem(i, heads)

                @pl.when(j < b)
                def _():
                    attend(j, [h0 + h for h in range(group)], False, pieces)

                @pl.when(j >= b)
                def _():
                    plain()

        for phase in range(3):
            def qkv_step(step, _, phase=phase):
                @pl.when(live)
                def _():
                    tick(phase, step)

                actions(step, range(phase * NK, (phase + 1) * NK))
                return 0

            acc[...] = jnp.zeros(acc.shape, jnp.float32)
            lax.fori_loop(phase * NK, (phase + 1) * NK, qkv_step, 0)

            @pl.when(live)
            def _(phase=phase):
                (put_q, put_k, put_v)[phase](b)

        @pl.when(live)
        def _():
            @pl.when(b > 0)
            def _():
                seen_copy(b - 1).wait_send()

            @pl.when(b + 1 < nb)
            def _():
                table_copy(b + 1).start()

            attention(b)
            seen_copy(b).start()
            forget()

            @pl.when(b + 1 < nb)
            def _():
                survey(b + 1)

        actions(MID, [MID])

        @pl.when(live)
        def _():
            seen_copy(b).wait_recv()

        def wo_step(step, _):
            @pl.when(live)
            def _():
                t = step - MID - 1
                g = b * TILES + 3 * NK + t
                s, ps = lax.rem(g, sz.slots), lax.rem(b, 2)
                next_tile(g, 3, 3 * NK + t)
                for i in range(2):
                    local(wo.at[:, pl.ds(0, wt)], wb.at[s, pl.ds(i * inner, inner), pl.ds(0, wt)], w_sem.at[s, i]).wait()
                for j in range(2):
                    n = t * 2 + j
                    p = jnp.where(n < 6, 0, jnp.where(n < 11, 1, 2))
                    bit = way(p, b, 0)[0]
                    go, stay = rows_of((1 - bit) * (m // 2), m // 2), rows_of(bit * (m // 2), m // 2)
                    here = jnp.concatenate([seen[go, :], seen[stay, :]], axis=0)
                    there = jnp.concatenate([seenp[ps, go, :], seenp[ps, stay, :]], axis=0)
                    c = slice(j * (wt // 2), (j + 1) * (wt // 2))
                    r = (jnp.dot(here, wb[s, 0:inner, c], preferred_element_type=jnp.float32)
                         + jnp.dot(there, wb[s, inner : 2 * inner, c], preferred_element_type=jnp.float32))
                    out = pl.ds(pl.multiple_of(n * (wt // 2), 128), wt // 2)
                    send1[:, out] = r[: m // 2].astype(send1.dtype)
                    keep[:, out] = r[m // 2 :]
                    normed(t, j * (m // 4), m // 4)

                @pl.when(b + 1 < nb)
                def _():
                    share(t).start()

                @pl.when(b + 2 < nb)
                def _():
                    x_copy(b + 2, t).start()

                for at, p in SENT.items():
                    @pl.when(step == at)
                    def _():
                        stage1(p, b).start()

            actions(step, range(MID + 1, STEPS))
            return 0

        lax.fori_loop(MID + 1, STEPS, wo_step, 0)
        return 0

    lax.fori_loop(0, nb + LAG, block, 0)
    seen_copy(jnp.int32(nb - 1)).wait_send()
    wx.wait_send()
    for p in range(3):
        fin_sent(p, jnp.int32(nb - 1))
        pass_on(3, p, jnp.int32(nb - 1)).wait_send()
    for b in range(nb):
        rest = y.at[pl.ds(b * m, m), pl.ds(other, half)]
        remote(rest, rest, d_send.at[0, 0], d_recv.at[b], mate).wait_recv()


def _angles(rows):
    half = HEAD // 2
    step = np.power(np.float32(THETA), -np.arange(half, dtype=np.float32) / np.float32(half)).astype(np.float32)
    angle = (np.arange(rows, dtype=np.float32)[:, None] * step).astype(np.float64)
    return np.concatenate([np.cos(angle), np.sin(angle)], -1).astype(np.float32)


def layer(sz, x, gain, wq, wk, wv, wo):
    low, f32 = x.dtype, jnp.float32
    m, inner, half = sz.m, sz.inner, sz.half
    vmem, dma = pltpu.VMEM, pltpu.SemaphoreType.DMA
    scratch = [
        vmem((NK, m, sz.kt), low),
        vmem((NK, m // 2, sz.kt), low),
        vmem((m // 2, 128), f32),
        vmem((sz.slots, max(sz.kt, 2 * inner), max(inner, sz.wt)), low),
        vmem((m, HEAD), f32),
        vmem((sz.heads, sz.rows, HEAD), low),
        vmem((sz.heads, HEAD + ONES, sz.rows), low),
        vmem((sz.heads, m, HEAD), low),
        vmem((m, inner), low),
        vmem((2, m, inner), low),
        vmem((m, inner), f32),
        vmem((sz.heads, HEAD + ONES, m), f32),
        vmem((sz.heads, 1, m), f32),
        vmem((m // 2, half), f32),
        vmem((m // 2, half), low),
        vmem((m // 2, half), low),
        vmem((m // 4, half), low),
        vmem((m // 4, half), low),
        vmem((m // 8, half), low),
        vmem((2, m // 8, half), low),
        vmem((m // 8, half), low),
        vmem((m // 8, half), low),
        dma((sz.slots, 2)), dma((NK,)), dma((NK,)), dma((NK,)), dma, dma((3,)), dma((2,)), dma, dma((2,)),
        dma((3, 3)), dma((3, 2, 3)), dma((6, 3)), dma((6, 2, 3)), dma((3,)), dma((4, 3)), dma((sz.blocks,)),
    ]
    hbm, here = pl.BlockSpec(memory_space=pl.ANY), pl.BlockSpec(memory_space=pltpu.VMEM)
    flops = 2 * sz.rows * sz.wide * 4 * inner + 2 * sz.rows * sz.rows * 2 * inner
    y, _ = pl.pallas_call(
        functools.partial(_kernel, sz),
        out_shape=[jax.ShapeDtypeStruct(x.shape, low), jax.ShapeDtypeStruct((inner, half), low)],
        in_specs=[hbm] * 6 + [here],
        out_specs=[hbm, hbm],
        scratch_shapes=scratch,
        compiler_params=pltpu.CompilerParams(collective_id=0, has_side_effects=True, vmem_limit_bytes=67043328),
        cost_estimate=pl.CostEstimate(flops=flops, bytes_accessed=4 * sz.blocks * inner * sz.wide * 2,
                                      transcendentals=sz.rows * sz.rows * sz.heads),
        name="decoder_attention",
    )(x, wq, wk, wv, wo, jnp.asarray(_angles(sz.rows)), gain.astype(f32).reshape(NK, 1, sz.kt))
    return y


def solution(mesh):
    def step(x, gain, wq, wk, wv, wo):
        sz = Sizes(rows=x.shape[0], wide=x.shape[1], heads=wq.shape[1] // HEAD)
        return layer(sz, x, gain, wq, wk, wv, wo)

    tokens, columns = P("dp", None), P(None, "tp")
    return jax.shard_map(
        step,
        mesh=mesh,
        in_specs=(tokens, P(None), columns, columns, columns, P("tp", None)),
        out_specs=tokens,
        check_vma=False,
    )
```

```python
import functools
from typing import NamedTuple

import jax
import jax.numpy as jnp
import numpy as np
from jax import lax
from jax.experimental import pallas as pl
from jax.experimental.pallas import tpu as pltpu
from jax.sharding import PartitionSpec as P

HEAD = 128
THETA = 10000
EPS = 1e-6
NEG = -1e30
HIDDEN = 2 * NEG
LOG2E = 1.4426950408889634
ONES = 16
NK = 8
NW = 8
TILES = 3 * NK + NW
MID = 3 * NK
STEPS = MID + 1 + NW


class Sizes(NamedTuple):
    rows: int
    wide: int
    heads: int
    m: int = 256
    slots: int = 5

    @property
    def blocks(self):
        return self.rows // self.m

    @property
    def inner(self):
        return self.heads * HEAD

    @property
    def half(self):
        return self.wide // 2

    @property
    def kt(self):
        return self.wide // NK

    @property
    def wt(self):
        return self.half // NW

    @property
    def parts(self):
        u = self.wt // 2
        return (0, 6 * u), (6 * u, 5 * u), (11 * u, 5 * u)


WHEN = {
    "add1": (10, 9, 11),
    "add2": (18, 15, 19),
    "add3": (24, 21, 23),
    "gather2": (30, 38, 27),
    "gather3": (47, 48, 43),
    "last": (76, 73, 63),
}
SENT = {MID + 3: 0, MID + 6: 1, MID + 8: 2}
LAG = max(max(w) for w in WHEN.values()) // STEPS + 1


def _held(sz):
    rows = sz.kt // 2
    pieces = [(0, (i // 2, slice(i % 2 * rows, (i % 2 + 1) * rows)), 0, rows, i * sz.inner, sz.inner) for i in range(2 * sz.slots)]
    tiles = [(r, c) for r in range(0, rows, sz.m) for c in range(2 * sz.slots * sz.inner, sz.wide, sz.kt)]
    pieces += [(1, (i,), r, sz.m, c, sz.kt) for i, (r, c) in enumerate(tiles[:NK])]
    n = sz.m // 2
    pieces += [(2, (2 * i + j,), r + j * n, n, c, sz.kt) for i, (r, c) in enumerate(tiles[NK:]) for j in range(2)]
    return pieces, rows


def _agenda(step):
    return [(stage, p, 1 + w[p] // STEPS) for stage, w in WHEN.items() for p in range(3) if w[p] % STEPS == step]


def _dot(a, b, ca, cb):
    return lax.dot_general(a, b, (((ca,), (cb,)), ((), ())), preferred_element_type=jnp.float32)


def _kernel(sz, x, wq, wk, wv, wo, angles, gain, y, wpart, xb, a, wb,
            ssq, table, kc, vt, q, seen, seenp, acc, mix, top, keep, send1, recv1, send2, recv2, send3, recv3, fin, xr,
            w_sem, x_sem, n_send, n_recv, t_sem, xr_sem, wx_sem, seen_send, seen_recv, s_sem, r_sem, g_send, g_recv, own_sem, d_send, d_recv, h_sem):
    m, nb, heads, inner, half, kt, wt = sz.m, sz.blocks, sz.heads, sz.inner, sz.half, sz.kt, sz.wt
    total = nb * TILES
    me = lax.axis_index("tp")
    core = lax.rem(me, 2)
    mate = me + 1 - 2 * core
    mine, other = pl.multiple_of(core * half, 128), pl.multiple_of((1 - core) * half, 128)

    def local(src, dst, sem):
        return pltpu.make_async_copy(src, dst, sem)

    def remote(src, dst, send, recv, to):
        return pltpu.make_async_remote_copy(src_ref=src, dst_ref=dst, send_sem=send, recv_sem=recv, device_id={"tp": to},
                                            device_id_type=pl.DeviceIdType.MESH)

    def rows_of(i, n):
        return pl.ds(pl.multiple_of(i, 16), n)


    def x_copy(b, k):
        at = rows_of(b * m + core * (m // 2), m // 2)
        return local(x.at[at, pl.ds(pl.multiple_of(k * kt, 128), kt)], xb.at[k], x_sem.at[k])

    def share(k):
        part = a.at[k, rows_of(core * (m // 2), m // 2)]
        return remote(part, part, n_send.at[k], n_recv.at[k], mate)

    wx = remote(wo.at[:, pl.ds(other, half)], wpart, wx_sem.at[0], wx_sem.at[1], mate)

    def fetch(g, j):
        s = lax.rem(g, sz.slots)

        def weight(w, k):
            local(w.at[rows_of(k * kt, kt)], wb.at[s], w_sem.at[s, 0]).start()

        def out(t):
            c = pl.multiple_of(t * wt, 128)
            local(wo.at[:, pl.ds(pl.multiple_of(mine + c, 128), wt)], wb.at[s, pl.ds(0, inner), pl.ds(0, wt)], w_sem.at[s, 0]).start()
            local(wpart.at[:, pl.ds(c, wt)], wb.at[s, pl.ds(inner, inner), pl.ds(0, wt)], w_sem.at[s, 1]).start()

        for i, w in enumerate((wq, wk, wv)):
            yield lambda w=w, i=i: weight(w, j - i * NK)
        yield lambda: out(j - 3 * NK)

    ahead = sz.slots - 1

    def next_tile(g, phase, step):
        last = (phase + 1) * NK - ahead
        here, there = list(fetch(g + ahead, step + ahead)), list(fetch(g + ahead, step + ahead - (TILES if phase == 3 else 0)))

        @pl.when(step < last)
        def _():
            here[phase]()

        @pl.when((step >= last) & (g + ahead < total))
        def _():
            if phase == 2:
                @pl.when(g == 3 * NK - ahead)
                def _():
                    wx.wait_recv()

            there[(phase + 1) % 4]()

    def table_copy(b):
        return local(angles.at[rows_of(b * m, m)], table, t_sem)


    def way(p, b, stage):
        axis = lax.rem(p + stage + b, 3)
        mask = 8 - 5 * axis + axis * axis
        bit = lax.rem(lax.div(me, mask), 2)
        return bit, me + mask * (1 - 2 * bit)

    def ways(p, b):
        return [way(p, b, stage) for stage in range(3)]

    def place(p, b, off, n):
        return rows_of(b * m + off, n), pl.ds(pl.multiple_of(mine + sz.parts[p][0], 128), sz.parts[p][1])

    def cols(p):
        return pl.ds(*sz.parts[p])

    def strips(p, body):
        c0, n = sz.parts[p]
        step = sz.wt // 2

        def one(i, _):
            body(pl.ds(pl.multiple_of(c0 + i * step, 128), step))
            return 0

        lax.fori_loop(0, n // step, one, 0)

    def wide(v):
        return v.astype(jnp.float32)

    def stage1(p, b):
        return remote(send1.at[:, cols(p)], recv1.at[:, cols(p)], s_sem.at[0, p], r_sem.at[0, lax.rem(b, 2), p],
                      ways(p, b)[0][1])

    def stage2(p, b):
        return remote(send2.at[:, cols(p)], recv2.at[:, cols(p)], s_sem.at[1, p], r_sem.at[1, lax.rem(b, 2), p],
                      ways(p, b)[1][1])

    def stage3(p, b):
        return remote(send3.at[:, cols(p)], recv3.at[lax.rem(b, 2), :, cols(p)], s_sem.at[2, p], r_sem.at[2, lax.rem(b, 2), p],
                      ways(p, b)[2][1])

    def offsets(p, b):
        (b1, _), (b2, _), (b3, _) = ways(p, b)
        return b1 * (m // 2), b1 * (m // 2) + b2 * (m // 4), b1 * (m // 2) + b2 * (m // 4) + b3 * (m // 8)

    def xr_copy(p, b):
        return local(x.at[place(p, b, offsets(p, b)[2], m // 8)], xr.at[:, cols(p)], xr_sem.at[p])

    def own_copy(p, b):
        return local(fin.at[:, cols(p)], y.at[place(p, b, offsets(p, b)[2], m // 8)], own_sem.at[p])

    def gather(kind, p, b):
        w, o = ways(p, b), offsets(p, b)
        n, axis = m // 8, (2, 1, 0, 1, 0, 0)[kind]
        if kind < 3:
            at, src = place(p, b, o[2], n), fin.at[:, cols(p)]
        else:
            if kind < 5:
                at = place(p, b, o[1] + (1 - w[2][0]) * n, n)
            else:
                at = place(p, b, o[0] + (1 - w[1][0]) * 2 * n, 2 * n)
            src = y.at[at]
        return remote(src, y.at[at], g_send.at[kind, p], g_recv.at[kind, lax.rem(b, 2), p], w[axis][1])

    def pass_on(kind, p, b):
        o = offsets(p, b)
        w = ways(p, b)
        if kind == 0:
            at, src = place(p, b, o[2], m // 8), fin.at[:, cols(p)]
        else:
            n = m // 8 << (kind - 1)
            base = (o[1], o[0], 0)[kind - 1]
            at = place(p, b, base + (1 - w[3 - kind][0]) * n, n)
            src = y.at[at]
        return remote(src, y.at[at], d_send.at[kind, p], d_recv.at[b], mate)

    def add1(p, b):
        w = ways(p, b)
        stage1(p, b).wait()
        h = m // 4
        go, stay = rows_of((1 - w[1][0]) * h, h), rows_of(w[1][0] * h, h)

        def body(c):
            send2[:, c] = (keep[go, c] + wide(recv1[go, c])).astype(send2.dtype)
            keep[stay, c] = keep[stay, c] + wide(recv1[stay, c])

        strips(p, body)
        stage2(p, b).start()

    def add2(p, b):
        w = ways(p, b)
        xr_copy(p, b).start()
        stage2(p, b).wait()
        h = m // 8
        base, go, stay = w[1][0] * (m // 4), (1 - w[2][0]) * h, w[2][0] * h

        def body(c):
            send3[:, c] = (keep[rows_of(base + go, h), c] + wide(recv2[rows_of(go, h), c])).astype(send3.dtype)
            keep[rows_of(base + stay, h), c] = keep[rows_of(base + stay, h), c] + wide(recv2[rows_of(stay, h), c])

        strips(p, body)
        stage3(p, b).start()

    def fin_sent(p, b):
        for kind in range(3):
            gather(kind, p, b).wait_send()
        own_copy(p, b).wait()
        pass_on(0, p, b).wait_send()

    def add3(p, b):
        s, w = lax.rem(b, 2), ways(p, b)

        @pl.when(b > 0)
        def _():
            fin_sent(p, b - 1)

        xr_copy(p, b).wait()
        stage3(p, b).wait()
        h = m // 8
        at = rows_of(w[1][0] * (m // 4) + w[2][0] * h, h)

        def body(c):
            fin[:, c] = (wide(xr[:, c]) + (keep[at, c] + wide(recv3[s, :, c]))).astype(fin.dtype)

        strips(p, body)
        for kind in range(3):
            gather(kind, p, b).start()
        own_copy(p, b).start()
        pass_on(0, p, b).start()

    def gather2(p, b):
        gather(0, p, b).wait_recv()
        for kind in (3, 4):
            gather(kind, p, b).start()
        pass_on(1, p, b).start()

    def gather3(p, b):
        gather(1, p, b).wait_recv()
        gather(3, p, b).wait_recv()
        gather(5, p, b).start()
        pass_on(2, p, b).start()
        gather(3, p, b).wait_send()
        pass_on(1, p, b).wait_send()

    def last(p, b):
        for kind in (2, 4, 5):
            gather(kind, p, b).wait_recv()
        for kind in (4, 5):
            gather(kind, p, b).wait_send()
        pass_on(2, p, b).wait_send()

        @pl.when(b > 0)
        def _():
            pass_on(3, p, b - 1).wait_send()

        pass_on(3, p, b).start()

    stages = {"add1": add1, "add2": add2, "add3": add3, "gather2": gather2, "gather3": gather3, "last": last}

    def act(stage, p, b):
        @pl.when((b >= 0) & (b < nb))
        def _():
            stages[stage](p, b)


    def survey(b):
        ssq[...] = jnp.zeros(ssq.shape, jnp.float32)

        def one(k, _):
            x_copy(b, k).wait()
            total = ssq[...]
            for c in range(0, kt, 128):
                v = wide(xb[k, :, c : c + 128])
                total = total + v * v
            ssq[...] = total
            return 0

        lax.fori_loop(0, NK, one, 0)
        total = jnp.sum(ssq[...], axis=1, keepdims=True)
        ssq[...] = jnp.broadcast_to(lax.rsqrt(total * (1 / sz.wide) + EPS), ssq.shape)

    def normed(k, first, n):
        at, to = slice(first, first + n), rows_of(core * (m // 2) + first, n)
        for c in range(0, kt, 128):
            v = wide(xb[k, at, c : c + 128]) * ssq[at, :] * gain[k, :, c : c + 128]
            a[k, to, c : c + 128] = v.astype(a.dtype)

    def turn(b, put):
        t = table[...]
        r = pltpu.roll(t, HEAD // 2, 1)
        low = lax.broadcasted_iota(jnp.int32, t.shape, 1) < HEAD // 2
        cos, sin = jnp.where(low, t, r), jnp.where(low, -r, t)
        for h in range(heads):
            v = wide(acc[:, h * HEAD : (h + 1) * HEAD].astype(q.dtype))
            put(h, (v * cos + pltpu.roll(v, HEAD // 2, 1) * sin).astype(q.dtype))

    def put_q(b):
        def put(h, v):
            q[h] = v
        turn(b, put)

    def put_k(b):
        def put(h, v):
            kc[h, rows_of(b * m, m), :] = v
        turn(b, put)

    def put_v(b):
        for h in range(heads):
            vt[h, 0:HEAD, pl.ds(pl.multiple_of(b * m, 128), m)] = acc[:, h * HEAD : (h + 1) * HEAD].T.astype(vt.dtype)

    e = HEAD**-0.5 * LOG2E
    group = min(heads, 4)

    def own(j):
        return pl.ds(pl.multiple_of(j * m, m), m)

    def score(j, h):
        return _dot(kc[h, own(j), :], q[h], 1, 1)

    def weigh(h, s, masked):
        if masked:
            ok = lax.broadcasted_iota(jnp.int32, s.shape, 0) <= lax.broadcasted_iota(jnp.int32, s.shape, 1)
            s = jnp.where(ok, s, HIDDEN)
        old = top[h]
        new = jnp.maximum(old, s.max(axis=0, keepdims=True))
        top[h] = new
        return jnp.exp2((s - new) * e).astype(vt.dtype), jnp.exp2((old - new) * e)

    def blend(j, h, w, k):
        mix[h] = mix[h] * k + _dot(vt[h, :, own(j)], w, 1, 0)

    def attend(j, hs, masked, pieces):
        n, r = len(pieces), len(hs)
        s, w = {}, {}

        def share(i):
            return range(r * i // n, r * (i + 1) // n) if 0 <= i < n else ()

        for i in range(n + 2):
            for h in share(i - 1):
                w[h] = weigh(hs[h], s.pop(h), masked)
            for h in share(i):
                s[h] = score(j, hs[h])
            for h in share(i - 2):
                blend(j, hs[h], *w.pop(h))
            if i < n:
                pieces[i]()

    def forget():
        top[...] = jnp.full(top.shape, NEG, jnp.float32)
        mix[...] = jnp.zeros(mix.shape, jnp.float32)

    def attention(b):
        attend(b, range(heads), True, [lambda: None] * 2)
        for h in range(heads):
            got = mix[h, 0:HEAD, :] * (1 / mix[h, HEAD : HEAD + 1, :])
            seen[:, h * HEAD : (h + 1) * HEAD] = got.T.astype(seen.dtype)

    def seen_copy(b):
        s = lax.rem(b, 2)
        return remote(seen, seenp.at[s], seen_send, seen_recv.at[s], mate)


    for k in range(NK):
        x_copy(0, k).start()
    for g in range(ahead):
        list(fetch(jnp.int32(g), g))[0]()
    table_copy(0).start()
    barrier = pltpu.get_barrier_semaphore()
    friends = [mate] + [way(0, 0, stage)[1] for stage in range(3)]
    for friend in friends:
        pl.semaphore_signal(barrier, inc=1, device_id={"tp": friend}, device_id_type=pl.DeviceIdType.MESH)

    survey(0)
    pl.semaphore_wait(barrier, len(friends))
    forget()

    def first(k, _):
        normed(k, 0, m // 2)
        share(k).start()
        x_copy(1, k).start()
        return 0

    lax.fori_loop(0, NK, first, 0)
    wx.start()
    for h in range(heads):
        vt[h, HEAD:, :] = jnp.ones((ONES, sz.rows), vt.dtype)

    def rest(b):
        return remote(y.at[pl.ds(b * m, m), pl.ds(other, half)], y.at[pl.ds(b * m, m), pl.ds(other, half)], d_send.at[0, 0], d_recv.at[b], mate)

    pieces, held = _held(sz)
    early = -(-held // m)

    def hold(i):
        buffer, at, r, n, c, w = pieces[i]
        return local(y.at[pl.ds(r, n), pl.ds(c, w)], (wb, a, xb)[buffer].at[at], h_sem.at[i])

    def block(b, _):
        live = b < nb

        @pl.when(b == nb)
        def _():
            for i in range(early):
                rest(i).wait_recv()
            for i in range(len(pieces)):
                hold(i).start()


        @pl.when(live)
        def _():
            table_copy(b).wait()

        def actions(step, steps):
            for at in steps:
                for stage, p, back in _agenda(at):
                    @pl.when(step == at)
                    def _():
                        act(stage, p, b - back)

        def tick(phase, step):
            g = b * TILES + step
            s, k = lax.rem(g, sz.slots), lax.rem(step, NK)
            next_tile(g, phase, step)
            if phase == 0:
                share(k).wait()
            local(wq.at[pl.ds(0, kt)], wb.at[s], w_sem.at[s, 0]).wait()

            n = 4

            def piece(i):
                c = slice(i * inner // n, (i + 1) * inner // n)
                acc[:, c] += jnp.dot(a[k], wb[s, :, c], preferred_element_type=jnp.float32)

            pieces = [functools.partial(piece, i) for i in range(n)]

            def plain():
                for one in pieces:
                    one()

            if phase == 0:
                plain()
            else:
                i = (step - NK) * group
                j, h0 = lax.div(i, heads), lax.rem(i, heads)

                @pl.when(j < b)
                def _():
                    attend(j, [h0 + h for h in range(group)], False, pieces)

                @pl.when(j >= b)
                def _():
                    plain()

        for phase in range(3):
            def qkv_step(step, _, phase=phase):
                @pl.when(live)
                def _():
                    tick(phase, step)

                actions(step, range(phase * NK, (phase + 1) * NK))
                return 0

            acc[...] = jnp.zeros(acc.shape, jnp.float32)
            lax.fori_loop(phase * NK, (phase + 1) * NK, qkv_step, 0)

            @pl.when(live)
            def _(phase=phase):
                (put_q, put_k, put_v)[phase](b)

        @pl.when(live)
        def _():
            @pl.when(b > 0)
            def _():
                seen_copy(b - 1).wait_send()

            @pl.when(b + 1 < nb)
            def _():
                table_copy(b + 1).start()

            attention(b)
            seen_copy(b).start()
            forget()

            @pl.when(b + 1 < nb)
            def _():
                survey(b + 1)

        actions(MID, [MID])

        @pl.when(live)
        def _():
            seen_copy(b).wait_recv()

        def wo_step(step, _):
            @pl.when(live)
            def _():
                t = step - MID - 1
                g = b * TILES + 3 * NK + t
                s, ps = lax.rem(g, sz.slots), lax.rem(b, 2)
                next_tile(g, 3, 3 * NK + t)
                for i in range(2):
                    local(wo.at[:, pl.ds(0, wt)], wb.at[s, pl.ds(i * inner, inner), pl.ds(0, wt)], w_sem.at[s, i]).wait()
                for j in range(2):
                    n = t * 2 + j
                    p = jnp.where(n < 6, 0, jnp.where(n < 11, 1, 2))
                    bit = way(p, b, 0)[0]
                    go, stay = rows_of((1 - bit) * (m // 2), m // 2), rows_of(bit * (m // 2), m // 2)
                    here = jnp.concatenate([seen[go, :], seen[stay, :]], axis=0)
                    there = jnp.concatenate([seenp[ps, go, :], seenp[ps, stay, :]], axis=0)
                    c = slice(j * (wt // 2), (j + 1) * (wt // 2))
                    r = (jnp.dot(here, wb[s, 0:inner, c], preferred_element_type=jnp.float32)
                         + jnp.dot(there, wb[s, inner : 2 * inner, c], preferred_element_type=jnp.float32))
                    out = pl.ds(pl.multiple_of(n * (wt // 2), 128), wt // 2)
                    send1[:, out] = r[: m // 2].astype(send1.dtype)
                    keep[:, out] = r[m // 2 :]
                    normed(t, j * (m // 4), m // 4)

                @pl.when(b + 1 < nb)
                def _():
                    share(t).start()

                @pl.when(b + 2 < nb)
                def _():
                    x_copy(b + 2, t).start()

                for at, p in SENT.items():
                    @pl.when(step == at)
                    def _():
                        stage1(p, b).start()

            actions(step, range(MID + 1, STEPS))
            return 0

        lax.fori_loop(MID + 1, STEPS, wo_step, 0)
        return 0

    lax.fori_loop(0, nb + LAG, block, 0)
    seen_copy(jnp.int32(nb - 1)).wait_send()
    wx.wait_send()
    for p in range(3):
        fin_sent(p, jnp.int32(nb - 1))
        pass_on(3, p, jnp.int32(nb - 1)).wait_send()
    for b in range(early, nb):
        rest(b).wait_recv()
    for i in range(len(pieces)):
        hold(i).wait()


def _collect(sz, y, xb, a, wb, out, ring, in_sem, out_sem, held_sem):
    pieces, first = _held(sz)
    slots, n = ring.shape[0], ring.shape[1]
    steps, ahead = (sz.rows - first) // n, slots // 2

    def held(i):
        buffer, at, r, k, c, w = pieces[i]
        return pltpu.make_async_copy((wb, a, xb)[buffer].at[at], out.at[pl.ds(r, k), pl.ds(c, w)], held_sem.at[i])

    def rows(i):
        return pl.ds(pl.multiple_of(first + i * n, n), n)

    def fetch(i):
        s = lax.rem(i, slots)
        return pltpu.make_async_copy(y.at[rows(i)], ring.at[s], in_sem.at[s])

    def store(i):
        s = lax.rem(i, slots)
        return pltpu.make_async_copy(ring.at[s], out.at[rows(i)], out_sem.at[s])

    for i in range(min(ahead, steps)):
        fetch(jnp.int32(i)).start()
    for i in range(len(pieces)):
        held(i).start()

    def one(i, _):
        fetch(i).wait()
        store(i).start()

        @pl.when(i + ahead < steps)
        def _():
            @pl.when(i + ahead >= slots)
            def _():
                store(i + ahead - slots).wait()

            fetch(i + ahead).start()
        return 0

    def end(i, _):
        store(i).wait()
        return 0

    lax.fori_loop(0, steps, one, 0)
    lax.fori_loop(max(steps - slots, 0), steps, end, 0)
    for i in range(len(pieces)):
        held(i).wait()


def _angles(rows):
    half = HEAD // 2
    step = np.power(np.float32(THETA), -np.arange(half, dtype=np.float32) / np.float32(half)).astype(np.float32)
    angle = (np.arange(rows, dtype=np.float32)[:, None] * step).astype(np.float64)
    return np.concatenate([np.cos(angle), np.sin(angle)], -1).astype(np.float32)


def layer(sz, x, gain, wq, wk, wv, wo):
    low, f32 = x.dtype, jnp.float32
    m, inner, half = sz.m, sz.inner, sz.half
    vmem, dma = pltpu.VMEM, pltpu.SemaphoreType.DMA
    pieces, held = _held(sz)
    kept = [
        vmem((NK, m // 2, sz.kt), low),
        vmem((NK, m, sz.kt), low),
        vmem((sz.slots, sz.kt, inner), low),
    ]
    scratch = [
        vmem((m // 2, 128), f32),
        vmem((m, HEAD), f32),
        vmem((sz.heads, sz.rows, HEAD), low),
        vmem((sz.heads, HEAD + ONES, sz.rows), low),
        vmem((sz.heads, m, HEAD), low),
        vmem((m, inner), low),
        vmem((2, m, inner), low),
        vmem((m, inner), f32),
        vmem((sz.heads, HEAD + ONES, m), f32),
        vmem((sz.heads, 1, m), f32),
        vmem((m // 2, half), f32),
        vmem((m // 2, half), low),
        vmem((m // 2, half), low),
        vmem((m // 4, half), low),
        vmem((m // 4, half), low),
        vmem((m // 8, half), low),
        vmem((2, m // 8, half), low),
        vmem((m // 8, half), low),
        vmem((m // 8, half), low),
        dma((sz.slots, 2)), dma((NK,)), dma((NK,)), dma((NK,)), dma, dma((3,)), dma((2,)), dma, dma((2,)),
        dma((3, 3)), dma((3, 2, 3)), dma((6, 3)), dma((6, 2, 3)), dma((3,)), dma((4, 3)), dma((sz.blocks,)), dma((len(pieces),)),
    ]
    hbm, here = pl.BlockSpec(memory_space=pl.ANY), pl.BlockSpec(memory_space=pltpu.VMEM)
    flops = 2 * sz.rows * sz.wide * 4 * inner + 2 * sz.rows * sz.rows * 2 * inner
    y, _, *kept = pl.pallas_call(
        functools.partial(_kernel, sz),
        out_shape=[jax.ShapeDtypeStruct(x.shape, low), jax.ShapeDtypeStruct((inner, half), low), *kept],
        in_specs=[hbm] * 6 + [here],
        out_specs=[hbm] * 2 + [here] * 3,
        scratch_shapes=scratch,
        compiler_params=pltpu.CompilerParams(collective_id=0, has_side_effects=True, vmem_limit_bytes=31 * 2**20),
        cost_estimate=pl.CostEstimate(flops=flops, bytes_accessed=4 * sz.blocks * inner * sz.wide * 2,
                                      transcendentals=sz.rows * sz.rows * sz.heads),
        name="decoder_attention",
    )(x, wq, wk, wv, wo, jnp.asarray(_angles(sz.rows)), gain.astype(f32).reshape(NK, 1, sz.kt))
    kept = [pltpu.with_memory_space_constraint(v, pltpu.MemorySpace.VMEM) for v in kept]
    ring, n = 12, min(64, sz.rows - held)
    return pl.pallas_call(
        functools.partial(_collect, sz),
        out_shape=jax.ShapeDtypeStruct(x.shape, low),
        in_specs=[hbm] * 4,
        out_specs=hbm,
        scratch_shapes=[vmem((ring, n, sz.wide), low), dma((ring,)), dma((ring,)), dma((len(pieces),))],
        compiler_params=pltpu.CompilerParams(vmem_limit_bytes=28 * 2**20),
        cost_estimate=pl.CostEstimate(flops=0, bytes_accessed=3 * sz.rows * sz.wide, transcendentals=0),
        name="collect",
    )(y, *kept)


def solution(mesh):
    def step(x, gain, wq, wk, wv, wo):
        sz = Sizes(rows=x.shape[0], wide=x.shape[1], heads=wq.shape[1] // HEAD)
        return layer(sz, x, gain, wq, wk, wv, wo)

    tokens, columns = P("dp", None), P(None, "tp")
    return jax.shard_map(
        step,
        mesh=mesh,
        in_specs=(tokens, P(None), columns, columns, columns, P("tp", None)),
        out_specs=tokens,
        check_vma=False,
    )
```

```python
import functools
from typing import NamedTuple

import jax
import jax.numpy as jnp
import numpy as np
from jax import lax
from jax.experimental import pallas as pl
from jax.experimental.pallas import tpu as pltpu
from jax.sharding import PartitionSpec as P

HEAD = 128
THETA = 10000
EPS = 1e-6
NEG = -1e30
HIDDEN = 2 * NEG
LOG2E = 1.4426950408889634
ONES = 16
NK = 8
NW = 8
TILES = 3 * NK + NW
MID = 3 * NK
STEPS = MID + 1 + NW


class Sizes(NamedTuple):
    rows: int
    wide: int
    heads: int
    m: int = 256
    slots: int = 5

    @property
    def blocks(self):
        return self.rows // self.m

    @property
    def inner(self):
        return self.heads * HEAD

    @property
    def half(self):
        return self.wide // 2

    @property
    def kt(self):
        return self.wide // NK

    @property
    def wt(self):
        return self.half // NW

    @property
    def parts(self):
        u = self.wt // 2
        return (0, 6 * u), (6 * u, 5 * u), (11 * u, 5 * u)


WHEN = {
    "add1": (10, 9, 11),
    "add2": (18, 15, 19),
    "add3": (24, 21, 23),
    "gather2": (30, 38, 27),
    "gather3": (47, 48, 43),
    "last": (76, 73, 63),
}
SENT = {MID + 3: 0, MID + 6: 1, MID + 8: 2}
LAG = max(max(w) for w in WHEN.values()) // STEPS + 1


def _held(sz):
    rows = sz.kt // 2
    pieces = [(5, (i // 2, slice(i % 2 * rows, (i % 2 + 1) * rows)), 0, rows, i * sz.inner, sz.inner) for i in range(2 * sz.slots)]
    tiles = [(r, c) for r in range(0, rows, sz.m) for c in range(2 * sz.slots * sz.inner, sz.wide, sz.kt)]
    pieces += [(4, (i,), r, sz.m, c, sz.kt) for i, (r, c) in enumerate(tiles[:NK])]
    n = sz.m // 2
    pieces += [(2, (2 * i + j,), r + j * n, n, c, sz.kt) for i, (r, c) in enumerate(tiles[NK:]) for j in range(2)]
    w = sz.wide // sz.heads
    if w <= sz.rows:
        pieces += [(3, (h, slice(0, HEAD), slice(0, w)), rows, HEAD, h * w, w) for h in range(sz.heads)]
        rows += HEAD
    now = len(pieces)
    pieces += [(i, (), rows, n, i * sz.half, sz.half) for i in range(2)]
    return pieces, now, rows + n


def _agenda(step):
    return [(stage, p, 1 + w[p] // STEPS) for stage, w in WHEN.items() for p in range(3) if w[p] % STEPS == step]


def _dot(a, b, ca, cb):
    return lax.dot_general(a, b, (((ca,), (cb,)), ((), ())), preferred_element_type=jnp.float32)


def _kernel(sz, x, wq, wk, wv, wo, angles, gain_in, y, wpart, send1, recv1, xb, vt, a, wb,
            gain, ssq, table, kc, q, seen, seenp, acc, mix, top, keep, send2, recv2, send3, recv3, fin, xr,
            w_sem, x_sem, n_send, n_recv, t_sem, xr_sem, wx_send, wx_recv, seen_send, seen_recv, s_sem, r_sem, g_send, g_recv, own_sem, d_send, d_recv, h_sem):
    m, nb, heads, inner, half, kt, wt = sz.m, sz.blocks, sz.heads, sz.inner, sz.half, sz.kt, sz.wt
    total = nb * TILES
    me = lax.axis_index("tp")
    core = lax.rem(me, 2)
    mate = me + 1 - 2 * core
    mine, other = pl.multiple_of(core * half, 128), pl.multiple_of((1 - core) * half, 128)

    def local(src, dst, sem):
        return pltpu.make_async_copy(src, dst, sem)

    def remote(src, dst, send, recv, to):
        return pltpu.make_async_remote_copy(src_ref=src, dst_ref=dst, send_sem=send, recv_sem=recv, device_id={"tp": to},
                                            device_id_type=pl.DeviceIdType.MESH)

    def rows_of(i, n):
        return pl.ds(pl.multiple_of(i, 16), n)


    def x_copy(b, k):
        at = rows_of(b * m + core * (m // 2), m // 2)
        return local(x.at[at, pl.ds(pl.multiple_of(k * kt, 128), kt)], xb.at[k], x_sem.at[k])

    def share(k):
        part = a.at[k, rows_of(core * (m // 2), m // 2)]
        return remote(part, part, n_send.at[k], n_recv.at[k], mate)

    def wx(t):
        c = pl.multiple_of(t * wt, 128)
        return remote(wo.at[:, pl.ds(pl.multiple_of(other + c, 128), wt)], wpart.at[:, pl.ds(c, wt)], wx_send.at[t], wx_recv.at[t], mate)

    def fetch(g, j):
        s = lax.rem(g, sz.slots)

        def weight(w, k):
            local(w.at[rows_of(k * kt, kt)], wb.at[s], w_sem.at[s, 0]).start()

        def out(t):
            c = pl.multiple_of(t * wt, 128)
            local(wo.at[:, pl.ds(pl.multiple_of(mine + c, 128), wt)], wb.at[s, pl.ds(0, inner), pl.ds(0, wt)], w_sem.at[s, 0]).start()
            local(wpart.at[:, pl.ds(c, wt)], wb.at[s, pl.ds(inner, inner), pl.ds(0, wt)], w_sem.at[s, 1]).start()

        for i, w in enumerate((wq, wk, wv)):
            yield lambda w=w, i=i: weight(w, j - i * NK)
        yield lambda: out(j - 3 * NK)

    ahead = sz.slots - 1

    def next_tile(g, phase, step):
        last = (phase + 1) * NK - ahead
        here, there = list(fetch(g + ahead, step + ahead)), list(fetch(g + ahead, step + ahead - (TILES if phase == 3 else 0)))

        def traded():
            @pl.when(g + ahead < TILES)
            def _():
                wx(g + ahead - 3 * NK).wait_recv()

        @pl.when(step < last)
        def _():
            if phase == 3:
                traded()
            here[phase]()

        @pl.when((step >= last) & (g + ahead < total))
        def _():
            if phase == 2:
                traded()
            there[(phase + 1) % 4]()

    def table_copy(b):
        return local(angles.at[rows_of(b * m, m)], table, t_sem)


    def way(p, b, stage):
        axis = lax.rem(p + stage + b, 3)
        mask = 8 - 5 * axis + axis * axis
        bit = lax.rem(lax.div(me, mask), 2)
        return bit, me + mask * (1 - 2 * bit)

    def ways(p, b):
        return [way(p, b, stage) for stage in range(3)]

    def place(p, b, off, n):
        return rows_of(b * m + off, n), pl.ds(pl.multiple_of(mine + sz.parts[p][0], 128), sz.parts[p][1])

    def cols(p):
        return pl.ds(*sz.parts[p])

    def strips(p, body):
        c0, n = sz.parts[p]
        step = sz.wt // 2

        def one(i, _):
            body(pl.ds(pl.multiple_of(c0 + i * step, 128), step))
            return 0

        lax.fori_loop(0, n // step, one, 0)

    def wide(v):
        return v.astype(jnp.float32)

    def stage1(p, b):
        return remote(send1.at[:, cols(p)], recv1.at[:, cols(p)], s_sem.at[0, p], r_sem.at[0, lax.rem(b, 2), p],
                      ways(p, b)[0][1])

    def stage2(p, b):
        return remote(send2.at[:, cols(p)], recv2.at[:, cols(p)], s_sem.at[1, p], r_sem.at[1, lax.rem(b, 2), p],
                      ways(p, b)[1][1])

    def stage3(p, b):
        return remote(send3.at[:, cols(p)], recv3.at[lax.rem(b, 2), :, cols(p)], s_sem.at[2, p], r_sem.at[2, lax.rem(b, 2), p],
                      ways(p, b)[2][1])

    def offsets(p, b):
        (b1, _), (b2, _), (b3, _) = ways(p, b)
        return b1 * (m // 2), b1 * (m // 2) + b2 * (m // 4), b1 * (m // 2) + b2 * (m // 4) + b3 * (m // 8)

    def xr_copy(p, b):
        return local(x.at[place(p, b, offsets(p, b)[2], m // 8)], xr.at[:, cols(p)], xr_sem.at[p])

    def own_copy(p, b):
        return local(fin.at[:, cols(p)], y.at[place(p, b, offsets(p, b)[2], m // 8)], own_sem.at[p])

    def gather(kind, p, b):
        w, o = ways(p, b), offsets(p, b)
        n, axis = m // 8, (2, 1, 0, 1, 0, 0)[kind]
        if kind < 3:
            at, src = place(p, b, o[2], n), fin.at[:, cols(p)]
        else:
            if kind < 5:
                at = place(p, b, o[1] + (1 - w[2][0]) * n, n)
            else:
                at = place(p, b, o[0] + (1 - w[1][0]) * 2 * n, 2 * n)
            src = y.at[at]
        return remote(src, y.at[at], g_send.at[kind, p], g_recv.at[kind, lax.rem(b, 2), p], w[axis][1])

    def pass_on(kind, p, b):
        o = offsets(p, b)
        w = ways(p, b)
        if kind == 0:
            at, src = place(p, b, o[2], m // 8), fin.at[:, cols(p)]
        else:
            n = m // 8 << (kind - 1)
            base = (o[1], o[0], 0)[kind - 1]
            at = place(p, b, base + (1 - w[3 - kind][0]) * n, n)
            src = y.at[at]
        return remote(src, y.at[at], d_send.at[kind, p], d_recv.at[b], mate)

    def add1(p, b):
        w = ways(p, b)
        stage1(p, b).wait()
        h = m // 4
        go, stay = rows_of((1 - w[1][0]) * h, h), rows_of(w[1][0] * h, h)

        def body(c):
            send2[:, c] = (keep[go, c] + wide(recv1[go, c])).astype(send2.dtype)
            keep[stay, c] = keep[stay, c] + wide(recv1[stay, c])

        strips(p, body)
        stage2(p, b).start()

    def add2(p, b):
        w = ways(p, b)
        xr_copy(p, b).start()
        stage2(p, b).wait()
        h = m // 8
        base, go, stay = w[1][0] * (m // 4), (1 - w[2][0]) * h, w[2][0] * h

        def body(c):
            send3[:, c] = (keep[rows_of(base + go, h), c] + wide(recv2[rows_of(go, h), c])).astype(send3.dtype)
            keep[rows_of(base + stay, h), c] = keep[rows_of(base + stay, h), c] + wide(recv2[rows_of(stay, h), c])

        strips(p, body)
        stage3(p, b).start()

    def fin_sent(p, b):
        for kind in range(3):
            gather(kind, p, b).wait_send()
        own_copy(p, b).wait()
        pass_on(0, p, b).wait_send()

    def add3(p, b):
        s, w = lax.rem(b, 2), ways(p, b)

        @pl.when(b > 0)
        def _():
            fin_sent(p, b - 1)

        xr_copy(p, b).wait()
        stage3(p, b).wait()
        h = m // 8
        at = rows_of(w[1][0] * (m // 4) + w[2][0] * h, h)

        def body(c):
            fin[:, c] = (wide(xr[:, c]) + (keep[at, c] + wide(recv3[s, :, c]))).astype(fin.dtype)

        strips(p, body)
        for kind in range(3):
            gather(kind, p, b).start()
        own_copy(p, b).start()
        pass_on(0, p, b).start()

    def gather2(p, b):
        gather(0, p, b).wait_recv()
        for kind in (3, 4):
            gather(kind, p, b).start()
        pass_on(1, p, b).start()

    def gather3(p, b):
        gather(1, p, b).wait_recv()
        gather(3, p, b).wait_recv()
        gather(5, p, b).start()
        pass_on(2, p, b).start()
        gather(3, p, b).wait_send()
        pass_on(1, p, b).wait_send()

    def last(p, b):
        for kind in (2, 4, 5):
            gather(kind, p, b).wait_recv()
        for kind in (4, 5):
            gather(kind, p, b).wait_send()
        pass_on(2, p, b).wait_send()

        @pl.when(b > 0)
        def _():
            pass_on(3, p, b - 1).wait_send()

        pass_on(3, p, b).start()

    stages = {"add1": add1, "add2": add2, "add3": add3, "gather2": gather2, "gather3": gather3, "last": last}

    def act(stage, p, b):
        @pl.when((b >= 0) & (b < nb))
        def _():
            stages[stage](p, b)


    def survey(b, meanwhile=None):
        ssq[...] = jnp.zeros(ssq.shape, jnp.float32)

        def one(k, _):
            x_copy(b, k).wait()
            total = ssq[...]
            for c in range(0, kt, 128):
                v = wide(xb[k, :, c : c + 128])
                total = total + v * v
            ssq[...] = total
            return 0

        if meanwhile is None:
            lax.fori_loop(0, NK, one, 0)
        else:
            lax.fori_loop(0, NK // 2, one, 0)
            meanwhile()
            lax.fori_loop(NK // 2, NK, one, 0)
        total = jnp.sum(ssq[...], axis=1, keepdims=True)
        ssq[...] = jnp.broadcast_to(lax.rsqrt(total * (1 / sz.wide) + EPS), ssq.shape)

    def normed(k, first, n):
        at, to = slice(first, first + n), rows_of(core * (m // 2) + first, n)
        for c in range(0, kt, 128):
            v = wide(xb[k, at, c : c + 128]) * ssq[at, :] * gain[k, :, c : c + 128]
            a[k, to, c : c + 128] = v.astype(a.dtype)

    def turn(b, put):
        t = table[...]
        r = pltpu.roll(t, HEAD // 2, 1)
        low = lax.broadcasted_iota(jnp.int32, t.shape, 1) < HEAD // 2
        cos, sin = jnp.where(low, t, r), jnp.where(low, -r, t)
        for h in range(heads):
            v = wide(acc[:, h * HEAD : (h + 1) * HEAD].astype(q.dtype))
            put(h, (v * cos + pltpu.roll(v, HEAD // 2, 1) * sin).astype(q.dtype))

    def put_q(b):
        def put(h, v):
            q[h] = v
        turn(b, put)

    def put_k(b):
        def put(h, v):
            kc[h, rows_of(b * m, m), :] = v
        turn(b, put)

    def put_v(b):
        for h in range(heads):
            vt[h, 0:HEAD, pl.ds(pl.multiple_of(b * m, 128), m)] = acc[:, h * HEAD : (h + 1) * HEAD].T.astype(vt.dtype)

    e = HEAD**-0.5 * LOG2E
    group = min(heads, 4)

    def own(j):
        return pl.ds(pl.multiple_of(j * m, m), m)

    def score(j, h):
        return _dot(kc[h, own(j), :], q[h], 1, 1)

    def weigh(h, s, masked):
        if masked:
            ok = lax.broadcasted_iota(jnp.int32, s.shape, 0) <= lax.broadcasted_iota(jnp.int32, s.shape, 1)
            s = jnp.where(ok, s, HIDDEN)
        old = top[h]
        new = jnp.maximum(old, s.max(axis=0, keepdims=True))
        top[h] = new
        return jnp.exp2((s - new) * e).astype(vt.dtype), jnp.exp2((old - new) * e)

    def blend(j, h, w, k):
        mix[h] = mix[h] * k + _dot(vt[h, :, own(j)], w, 1, 0)

    def attend(j, hs, masked, pieces):
        n, r = len(pieces), len(hs)
        s, w = {}, {}

        def share(i):
            return range(r * i // n, r * (i + 1) // n) if 0 <= i < n else ()

        for i in range(n + 2):
            for h in share(i - 1):
                w[h] = weigh(hs[h], s.pop(h), masked)
            for h in share(i):
                s[h] = score(j, hs[h])
            for h in share(i - 2):
                blend(j, hs[h], *w.pop(h))
            if i < n:
                pieces[i]()

    def forget():
        top[...] = jnp.full(top.shape, NEG, jnp.float32)
        mix[...] = jnp.zeros(mix.shape, jnp.float32)

    def attention(b):
        attend(b, range(heads), True, [lambda: None] * 2)
        for h in range(heads):
            got = mix[h, 0:HEAD, :] * (1 / mix[h, HEAD : HEAD + 1, :])
            seen[:, h * HEAD : (h + 1) * HEAD] = got.T.astype(seen.dtype)

    def seen_copy(b):
        s = lax.rem(b, 2)
        return remote(seen, seenp.at[s], seen_send, seen_recv.at[s], mate)


    for k in range(NK):
        x_copy(0, k).start()
    barrier = pltpu.get_barrier_semaphore()
    friends = [mate] + [way(0, 0, stage)[1] for stage in range(3)]
    for friend in friends:
        pl.semaphore_signal(barrier, inc=1, device_id={"tp": friend}, device_id_type=pl.DeviceIdType.MESH)

    for h in range(heads):
        vt[h, HEAD:, :] = jnp.ones((ONES, sz.rows), vt.dtype)
    whole = wide(gain_in[...])
    for i in range(sz.wide // 128):
        gain[i * 128 // kt, :, i * 128 % kt : i * 128 % kt + 128] = whole[i : i + 1, :]

    def weights():
        for g in range(ahead):
            list(fetch(jnp.int32(g), g))[0]()
        table_copy(0).start()

    survey(0, weights)
    pl.semaphore_wait(barrier, len(friends))
    forget()

    def first(k, _):
        normed(k, 0, m // 2)
        share(k).start()
        x_copy(1, k).start()
        return 0

    lax.fori_loop(0, NK, first, 0)

    def rest(b):
        return remote(y.at[pl.ds(b * m, m), pl.ds(other, half)], y.at[pl.ds(b * m, m), pl.ds(other, half)], d_send.at[0, 0], d_recv.at[b], mate)

    pieces, now, held = _held(sz)
    early = -(-held // m)

    def hold(i):
        buffer, at, r, n, c, w = pieces[i]
        return local(y.at[pl.ds(r, n), pl.ds(c, w)], (send1, recv1, xb, vt, a, wb)[buffer].at[at], h_sem.at[i])

    def block(b, _):
        live = b < nb

        @pl.when(b == nb)
        def _():
            for i in range(early):
                rest(i).wait_recv()
            for i in range(now):
                hold(i).start()
            seen_copy(b - 1).wait_send()
            for t in range(NW):
                wx(t).wait_send()

        @pl.when(b == nb + 1)
        def _():
            for i in range(len(pieces)):
                hold(i).wait()

        @pl.when(live)
        def _():
            table_copy(b).wait()

        def actions(step, steps):
            for at in steps:
                for stage, p, back in _agenda(at):
                    @pl.when(step == at)
                    def _():
                        act(stage, p, b - back)

        def tick(phase, step):
            g = b * TILES + step
            s, k = lax.rem(g, sz.slots), lax.rem(step, NK)
            next_tile(g, phase, step)
            if phase == 0:
                @pl.when(g < NW)
                def _():
                    wx(g).start()

                share(k).wait()
            local(wq.at[pl.ds(0, kt)], wb.at[s], w_sem.at[s, 0]).wait()

            n = 4

            def piece(i):
                c = slice(i * inner // n, (i + 1) * inner // n)
                acc[:, c] += jnp.dot(a[k], wb[s, :, c], preferred_element_type=jnp.float32)

            pieces = [functools.partial(piece, i) for i in range(n)]

            def plain():
                for one in pieces:
                    one()

            if phase == 0:
                plain()
            else:
                i = (step - NK) * group
                j, h0 = lax.div(i, heads), lax.rem(i, heads)

                @pl.when(j < b)
                def _():
                    attend(j, [h0 + h for h in range(group)], False, pieces)

                @pl.when(j >= b)
                def _():
                    plain()

        for phase in range(3):
            def qkv_step(step, _, phase=phase):
                @pl.when(live)
                def _():
                    tick(phase, step)

                actions(step, range(phase * NK, (phase + 1) * NK))
                return 0

            acc[...] = jnp.zeros(acc.shape, jnp.float32)
            lax.fori_loop(phase * NK, (phase + 1) * NK, qkv_step, 0)
            if phase == 1:
                @pl.when(b == nb)
                def _():
                    for i in range(now, len(pieces)):
                        hold(i).start()

            @pl.when(live)
            def _(phase=phase):
                (put_q, put_k, put_v)[phase](b)

        @pl.when(live)
        def _():
            @pl.when(b > 0)
            def _():
                seen_copy(b - 1).wait_send()

            @pl.when(b + 1 < nb)
            def _():
                table_copy(b + 1).start()

            attention(b)
            seen_copy(b).start()
            forget()

            @pl.when(b + 1 < nb)
            def _():
                survey(b + 1)

        actions(MID, [MID])

        @pl.when(live)
        def _():
            seen_copy(b).wait_recv()

        def wo_step(step, _):
            @pl.when(live)
            def _():
                t = step - MID - 1
                g = b * TILES + 3 * NK + t
                s, ps = lax.rem(g, sz.slots), lax.rem(b, 2)
                next_tile(g, 3, 3 * NK + t)
                for i in range(2):
                    local(wo.at[:, pl.ds(0, wt)], wb.at[s, pl.ds(i * inner, inner), pl.ds(0, wt)], w_sem.at[s, i]).wait()
                for j in range(2):
                    n = t * 2 + j
                    p = jnp.where(n < 6, 0, jnp.where(n < 11, 1, 2))
                    bit = way(p, b, 0)[0]
                    go, stay = rows_of((1 - bit) * (m // 2), m // 2), rows_of(bit * (m // 2), m // 2)
                    here = jnp.concatenate([seen[go, :], seen[stay, :]], axis=0)
                    there = jnp.concatenate([seenp[ps, go, :], seenp[ps, stay, :]], axis=0)
                    c = slice(j * (wt // 2), (j + 1) * (wt // 2))
                    r = (jnp.dot(here, wb[s, 0:inner, c], preferred_element_type=jnp.float32)
                         + jnp.dot(there, wb[s, inner : 2 * inner, c], preferred_element_type=jnp.float32))
                    out = pl.ds(pl.multiple_of(n * (wt // 2), 128), wt // 2)
                    send1[:, out] = r[: m // 2].astype(send1.dtype)
                    keep[:, out] = r[m // 2 :]
                    normed(t, j * (m // 4), m // 4)

                @pl.when(b + 1 < nb)
                def _():
                    share(t).start()

                @pl.when(b + 2 < nb)
                def _():
                    x_copy(b + 2, t).start()

                for at, p in SENT.items():
                    @pl.when(step == at)
                    def _():
                        stage1(p, b).start()

            actions(step, range(MID + 1, STEPS))
            return 0

        lax.fori_loop(MID + 1, STEPS, wo_step, 0)
        return 0

    lax.fori_loop(0, nb + LAG, block, 0)
    for p in range(3):
        fin_sent(p, jnp.int32(nb - 1))
        pass_on(3, p, jnp.int32(nb - 1)).wait_send()
    for b in range(early, nb):
        rest(b).wait_recv()


def _collect(sz, y, send1, recv1, xb, vt, a, wb, out, ring, in_sem, out_sem, held_sem):
    pieces, _, first = _held(sz)
    slots, n = ring.shape[0], ring.shape[1]
    steps, ahead = (sz.rows - first) // n, slots // 2

    def held(i):
        buffer, at, r, k, c, w = pieces[i]
        return pltpu.make_async_copy((send1, recv1, xb, vt, a, wb)[buffer].at[at], out.at[pl.ds(r, k), pl.ds(c, w)], held_sem.at[i])

    def rows(i):
        return pl.ds(pl.multiple_of(first + i * n, n), n)

    def fetch(i):
        s = lax.rem(i, slots)
        return pltpu.make_async_copy(y.at[rows(i)], ring.at[s], in_sem.at[s])

    def store(i):
        s = lax.rem(i, slots)
        return pltpu.make_async_copy(ring.at[s], out.at[rows(i)], out_sem.at[s])

    for i in range(min(ahead, steps)):
        fetch(jnp.int32(i)).start()
    for i in range(len(pieces)):
        held(i).start()

    def one(i, _):
        fetch(i).wait()
        store(i).start()

        @pl.when(i + ahead < steps)
        def _():
            @pl.when(i + ahead >= slots)
            def _():
                store(i + ahead - slots).wait()

            fetch(i + ahead).start()
        return 0

    def end(i, _):
        store(i).wait()
        return 0

    lax.fori_loop(0, steps, one, 0)
    lax.fori_loop(max(steps - slots, 0), steps, end, 0)
    for i in range(len(pieces)):
        held(i).wait()


def _angles(rows):
    half = HEAD // 2
    step = np.power(np.float32(THETA), -np.arange(half, dtype=np.float32) / np.float32(half)).astype(np.float32)
    angle = (np.arange(rows, dtype=np.float32)[:, None] * step).astype(np.float64)
    return np.concatenate([np.cos(angle), np.sin(angle)], -1).astype(np.float32)


def layer(sz, x, gain, wq, wk, wv, wo):
    low, f32 = x.dtype, jnp.float32
    m, inner, half = sz.m, sz.inner, sz.half
    vmem, dma = pltpu.VMEM, pltpu.SemaphoreType.DMA
    pieces, _, held = _held(sz)
    kept = [
        vmem((m // 2, half), low),
        vmem((m // 2, half), low),
        vmem((NK, m // 2, sz.kt), low),
        vmem((sz.heads, HEAD + ONES, sz.rows), low),
        vmem((NK, m, sz.kt), low),
        vmem((sz.slots, sz.kt, inner), low),
    ]
    scratch = [
        vmem((NK, 1, sz.kt), f32),
        vmem((m // 2, 128), f32),
        vmem((m, HEAD), f32),
        vmem((sz.heads, sz.rows, HEAD), low),
        vmem((sz.heads, m, HEAD), low),
        vmem((m, inner), low),
        vmem((2, m, inner), low),
        vmem((m, inner), f32),
        vmem((sz.heads, HEAD + ONES, m), f32),
        vmem((sz.heads, 1, m), f32),
        vmem((m // 2, half), f32),
        vmem((m // 4, half), low),
        vmem((m // 4, half), low),
        vmem((m // 8, half), low),
        vmem((2, m // 8, half), low),
        vmem((m // 8, half), low),
        vmem((m // 8, half), low),
        dma((sz.slots, 2)), dma((NK,)), dma((NK,)), dma((NK,)), dma, dma((3,)), dma((NW,)), dma((NW,)), dma, dma((2,)),
        dma((3, 3)), dma((3, 2, 3)), dma((6, 3)), dma((6, 2, 3)), dma((3,)), dma((4, 3)), dma((sz.blocks,)), dma((len(pieces),)),
    ]
    hbm, here = pl.BlockSpec(memory_space=pl.ANY), pl.BlockSpec(memory_space=pltpu.VMEM)
    flops = 2 * sz.rows * sz.wide * 4 * inner + 2 * sz.rows * sz.rows * 2 * inner
    y, _, *kept = pl.pallas_call(
        functools.partial(_kernel, sz),
        out_shape=[jax.ShapeDtypeStruct(x.shape, low), jax.ShapeDtypeStruct((inner, half), low), *kept],
        in_specs=[hbm] * 6 + [here],
        out_specs=[hbm] * 2 + [here] * 6,
        scratch_shapes=scratch,
        compiler_params=pltpu.CompilerParams(collective_id=0, has_side_effects=True, vmem_limit_bytes=21 * 2**20),
        cost_estimate=pl.CostEstimate(flops=flops, bytes_accessed=4 * sz.blocks * inner * sz.wide * 2,
                                      transcendentals=sz.rows * sz.rows * sz.heads),
        name="decoder_attention",
    )(x, wq, wk, wv, wo, jnp.asarray(_angles(sz.rows)), gain.reshape(sz.wide // 128, 128))
    kept = [pltpu.with_memory_space_constraint(v, pltpu.MemorySpace.VMEM) for v in kept]
    ring, n = 8, min(64, sz.rows - held)
    return pl.pallas_call(
        functools.partial(_collect, sz),
        out_shape=jax.ShapeDtypeStruct(x.shape, low),
        in_specs=[hbm] * 7,
        out_specs=hbm,
        scratch_shapes=[vmem((ring, n, sz.wide), low), dma((ring,)), dma((ring,)), dma((len(pieces),))],
        compiler_params=pltpu.CompilerParams(vmem_limit_bytes=18 * 2**20),
        cost_estimate=pl.CostEstimate(flops=0, bytes_accessed=3 * sz.rows * sz.wide, transcendentals=0),
        name="collect",
    )(y, *kept)


def solution(mesh):
    def step(x, gain, wq, wk, wv, wo):
        sz = Sizes(rows=x.shape[0], wide=x.shape[1], heads=wq.shape[1] // HEAD)
        return layer(sz, x, gain, wq, wk, wv, wo)

    tokens, columns = P("dp", None), P(None, "tp")
    return jax.shard_map(
        step,
        mesh=mesh,
        in_specs=(tokens, P(None), columns, columns, columns, P("tp", None)),
        out_specs=tokens,
        check_vma=False,
    )
```

```python
import functools
from typing import NamedTuple

import jax
import jax.numpy as jnp
import numpy as np
from jax import lax
from jax.experimental import pallas as pl
from jax.experimental.pallas import tpu as pltpu
from jax.sharding import PartitionSpec as P

HEAD = 128
THETA = 10000
EPS = 1e-6
NEG = -1e30
HIDDEN = 2 * NEG
LOG2E = 1.4426950408889634
ONES = 16
NK = 8
NW = 8
TILES = 3 * NK + NW
MID = 3 * NK
STEPS = MID + 1 + NW


class Sizes(NamedTuple):
    rows: int
    wide: int
    heads: int
    m: int = 256
    slots: int = 5

    @property
    def blocks(self):
        return self.rows // self.m

    @property
    def inner(self):
        return self.heads * HEAD

    @property
    def half(self):
        return self.wide // 2

    @property
    def kt(self):
        return self.wide // NK

    @property
    def wt(self):
        return self.half // NW

    @property
    def parts(self):
        u = self.wt // 2
        return (0, 6 * u), (6 * u, 5 * u), (11 * u, 5 * u)


WHEN = {
    "add1": (8, 9, 11),
    "add2": (17, 15, 18),
    "add3": (24, 21, 23),
    "gather2": (29, 30, 27),
    "gather3": (46, 48, 44),
    "last": (61, 59, 58),
}
SENT = {MID + 3: 0, MID + 6: 1, MID + 8: 2}
LAG = max(max(w) for w in WHEN.values()) // STEPS + 1


def _held(sz):
    rows = sz.kt // 2
    pieces = [(5, (i // 2, slice(i % 2 * rows, (i % 2 + 1) * rows)), 0, rows, i * sz.inner, sz.inner) for i in range(2 * sz.slots)]
    tiles = [(r, c) for r in range(0, rows, sz.m) for c in range(2 * sz.slots * sz.inner, sz.wide, sz.kt)]
    pieces += [(4, (i,), r, sz.m, c, sz.kt) for i, (r, c) in enumerate(tiles[:NK])]
    n = sz.m // 2
    pieces += [(2, (2 * i + j,), r + j * n, n, c, sz.kt) for i, (r, c) in enumerate(tiles[NK:]) for j in range(2)]
    w = sz.wide // sz.heads
    if w <= sz.rows:
        pieces += [(3, (h, slice(0, HEAD), slice(0, w)), rows, HEAD, h * w, w) for h in range(sz.heads)]
        rows += HEAD
    now = len(pieces)
    pieces += [(i, (), rows, n, i * sz.half, sz.half) for i in range(2)]
    return pieces, now, rows + n


def _agenda(step):
    return [(stage, p, 1 + w[p] // STEPS) for stage, w in WHEN.items() for p in range(3) if w[p] % STEPS == step]


def _dot(a, b, ca, cb):
    return lax.dot_general(a, b, (((ca,), (cb,)), ((), ())), preferred_element_type=jnp.float32)


def _kernel(sz, x, wq, wk, wv, wo, angles, gain_in, y, wpart, send1, recv1, xb, vt, a, wb,
            gain, ssq, table, kc, q, seen, seenp, acc, mix, top, keep, send2, recv2, send3, recv3, fin, xr,
            w_sem, x_sem, n_send, n_recv, t_sem, xr_sem, wx_send, wx_recv, seen_send, seen_recv, s_sem, r_sem, g_send, g_recv, own_sem, d_send, d_recv, h_sem):
    m, nb, heads, inner, half, kt, wt = sz.m, sz.blocks, sz.heads, sz.inner, sz.half, sz.kt, sz.wt
    total = nb * TILES
    me = lax.axis_index("tp")
    core = lax.rem(me, 2)
    mate = me + 1 - 2 * core
    mine, other = pl.multiple_of(core * half, 128), pl.multiple_of((1 - core) * half, 128)

    def local(src, dst, sem):
        return pltpu.make_async_copy(src, dst, sem)

    def remote(src, dst, send, recv, to):
        return pltpu.make_async_remote_copy(src_ref=src, dst_ref=dst, send_sem=send, recv_sem=recv, device_id={"tp": to},
                                            device_id_type=pl.DeviceIdType.MESH)

    def rows_of(i, n):
        return pl.ds(pl.multiple_of(i, 16), n)


    def x_copy(b, k):
        at = rows_of(b * m + core * (m // 2), m // 2)
        return local(x.at[at, pl.ds(pl.multiple_of(k * kt, 128), kt)], xb.at[k], x_sem.at[k])

    def share(k):
        part = a.at[k, rows_of(core * (m // 2), m // 2)]
        return remote(part, part, n_send.at[k], n_recv.at[k], mate)

    def wx(t):
        c = pl.multiple_of(t * wt, 128)
        return remote(wo.at[:, pl.ds(pl.multiple_of(other + c, 128), wt)], wpart.at[:, pl.ds(c, wt)], wx_send.at[t], wx_recv.at[t], mate)

    def fetch(g, j):
        s = lax.rem(g, sz.slots)

        def weight(w, k):
            local(w.at[rows_of(k * kt, kt)], wb.at[s], w_sem.at[s, 0]).start()

        def out(t):
            c = pl.multiple_of(t * wt, 128)
            local(wo.at[:, pl.ds(pl.multiple_of(mine + c, 128), wt)], wb.at[s, pl.ds(0, inner), pl.ds(0, wt)], w_sem.at[s, 0]).start()
            local(wpart.at[:, pl.ds(c, wt)], wb.at[s, pl.ds(inner, inner), pl.ds(0, wt)], w_sem.at[s, 1]).start()

        for i, w in enumerate((wq, wk, wv)):
            yield lambda w=w, i=i: weight(w, j - i * NK)
        yield lambda: out(j - 3 * NK)

    ahead = sz.slots - 1

    def next_tile(g, phase, step):
        last = (phase + 1) * NK - ahead
        here, there = list(fetch(g + ahead, step + ahead)), list(fetch(g + ahead, step + ahead - (TILES if phase == 3 else 0)))

        def traded():
            @pl.when(g + ahead < TILES)
            def _():
                wx(g + ahead - 3 * NK).wait_recv()

        @pl.when(step < last)
        def _():
            if phase == 3:
                traded()
            here[phase]()

        @pl.when((step >= last) & (g + ahead < total))
        def _():
            if phase == 2:
                traded()
            there[(phase + 1) % 4]()

    def table_copy(b):
        return local(angles.at[rows_of(b * m, m)], table, t_sem)


    def way(p, b, stage):
        axis = lax.rem(p + stage + b, 3)
        mask = 8 - 5 * axis + axis * axis
        bit = lax.rem(lax.div(me, mask), 2)
        return bit, me + mask * (1 - 2 * bit)

    def ways(p, b):
        return [way(p, b, stage) for stage in range(3)]

    def place(p, b, off, n):
        return rows_of(b * m + off, n), pl.ds(pl.multiple_of(mine + sz.parts[p][0], 128), sz.parts[p][1])

    def cols(p):
        return pl.ds(*sz.parts[p])

    def strips(p, body):
        c0, n = sz.parts[p]
        step = sz.wt // 2

        def one(i, _):
            body(pl.ds(pl.multiple_of(c0 + i * step, 128), step))
            return 0

        lax.fori_loop(0, n // step, one, 0)

    def wide(v):
        return v.astype(jnp.float32)

    def stage1(p, b):
        return remote(send1.at[:, cols(p)], recv1.at[:, cols(p)], s_sem.at[0, p], r_sem.at[0, lax.rem(b, 2), p],
                      ways(p, b)[0][1])

    def stage2(p, b):
        return remote(send2.at[:, cols(p)], recv2.at[:, cols(p)], s_sem.at[1, p], r_sem.at[1, lax.rem(b, 2), p],
                      ways(p, b)[1][1])

    def stage3(p, b):
        return remote(send3.at[:, cols(p)], recv3.at[lax.rem(b, 2), :, cols(p)], s_sem.at[2, p], r_sem.at[2, lax.rem(b, 2), p],
                      ways(p, b)[2][1])

    def offsets(p, b):
        (b1, _), (b2, _), (b3, _) = ways(p, b)
        return b1 * (m // 2), b1 * (m // 2) + b2 * (m // 4), b1 * (m // 2) + b2 * (m // 4) + b3 * (m // 8)

    def xr_copy(p, b):
        return local(x.at[place(p, b, offsets(p, b)[2], m // 8)], xr.at[:, cols(p)], xr_sem.at[p])

    def own_copy(p, b):
        return local(fin.at[:, cols(p)], y.at[place(p, b, offsets(p, b)[2], m // 8)], own_sem.at[p])

    def gather(kind, p, b):
        w, o = ways(p, b), offsets(p, b)
        n, axis = m // 8, (2, 1, 0, 1, 0, 0)[kind]
        if kind < 3:
            at, src = place(p, b, o[2], n), fin.at[:, cols(p)]
        else:
            if kind < 5:
                at = place(p, b, o[1] + (1 - w[2][0]) * n, n)
            else:
                at = place(p, b, o[0] + (1 - w[1][0]) * 2 * n, 2 * n)
            src = y.at[at]
        return remote(src, y.at[at], g_send.at[kind, p], g_recv.at[kind, lax.rem(b, 2), p], w[axis][1])

    def pass_on(kind, p, b):
        o = offsets(p, b)
        w = ways(p, b)
        if kind == 0:
            at, src = place(p, b, o[2], m // 8), fin.at[:, cols(p)]
        else:
            n = m // 8 << (kind - 1)
            base = (o[1], o[0], 0)[kind - 1]
            at = place(p, b, base + (1 - w[3 - kind][0]) * n, n)
            src = y.at[at]
        return remote(src, y.at[at], d_send.at[kind, p], d_recv.at[b], mate)

    def add1(p, b):
        w = ways(p, b)
        stage1(p, b).wait()
        h = m // 4
        go, stay = rows_of((1 - w[1][0]) * h, h), rows_of(w[1][0] * h, h)

        def body(c):
            send2[:, c] = (keep[go, c] + wide(recv1[go, c])).astype(send2.dtype)
            keep[stay, c] = keep[stay, c] + wide(recv1[stay, c])

        strips(p, body)
        stage2(p, b).start()

    def add2(p, b):
        w = ways(p, b)
        xr_copy(p, b).start()
        stage2(p, b).wait()
        h = m // 8
        base, go, stay = w[1][0] * (m // 4), (1 - w[2][0]) * h, w[2][0] * h

        def body(c):
            send3[:, c] = (keep[rows_of(base + go, h), c] + wide(recv2[rows_of(go, h), c])).astype(send3.dtype)
            keep[rows_of(base + stay, h), c] = keep[rows_of(base + stay, h), c] + wide(recv2[rows_of(stay, h), c])

        strips(p, body)
        stage3(p, b).start()

    def fin_sent(p, b):
        for kind in range(3):
            gather(kind, p, b).wait_send()
        own_copy(p, b).wait()
        pass_on(0, p, b).wait_send()

    def add3(p, b):
        s, w = lax.rem(b, 2), ways(p, b)

        @pl.when(b > 0)
        def _():
            fin_sent(p, b - 1)

        xr_copy(p, b).wait()
        stage3(p, b).wait()
        h = m // 8
        at = rows_of(w[1][0] * (m // 4) + w[2][0] * h, h)

        def body(c):
            fin[:, c] = (wide(xr[:, c]) + (keep[at, c] + wide(recv3[s, :, c]))).astype(fin.dtype)

        strips(p, body)
        for kind in range(3):
            gather(kind, p, b).start()
        own_copy(p, b).start()
        pass_on(0, p, b).start()

    def gather2(p, b):
        gather(0, p, b).wait_recv()
        for kind in (3, 4):
            gather(kind, p, b).start()
        pass_on(1, p, b).start()

    def gather3(p, b):
        gather(1, p, b).wait_recv()
        gather(3, p, b).wait_recv()
        gather(5, p, b).start()
        pass_on(2, p, b).start()
        gather(3, p, b).wait_send()
        pass_on(1, p, b).wait_send()

    def last(p, b):
        for kind in (2, 4, 5):
            gather(kind, p, b).wait_recv()
        for kind in (4, 5):
            gather(kind, p, b).wait_send()
        pass_on(2, p, b).wait_send()

        @pl.when(b > 0)
        def _():
            pass_on(3, p, b - 1).wait_send()

        pass_on(3, p, b).start()

    stages = {"add1": add1, "add2": add2, "add3": add3, "gather2": gather2, "gather3": gather3, "last": last}

    def act(stage, p, b):
        @pl.when((b >= 0) & (b < nb))
        def _():
            stages[stage](p, b)


    def survey(b, meanwhile=None):
        ssq[...] = jnp.zeros(ssq.shape, jnp.float32)

        def one(k, _):
            x_copy(b, k).wait()
            total = ssq[...]
            for c in range(0, kt, 128):
                v = wide(xb[k, :, c : c + 128])
                total = total + v * v
            ssq[...] = total
            return 0

        if meanwhile is None:
            lax.fori_loop(0, NK, one, 0)
        else:
            lax.fori_loop(0, NK // 2, one, 0)
            meanwhile()
            lax.fori_loop(NK // 2, NK, one, 0)
        total = jnp.sum(ssq[...], axis=1, keepdims=True)
        ssq[...] = jnp.broadcast_to(lax.rsqrt(total * (1 / sz.wide) + EPS), ssq.shape)

    def normed(k, first, n):
        at, to = slice(first, first + n), rows_of(core * (m // 2) + first, n)
        for c in range(0, kt, 128):
            v = wide(xb[k, at, c : c + 128]) * ssq[at, :] * gain[k, :, c : c + 128]
            a[k, to, c : c + 128] = v.astype(a.dtype)

    def turn(b, put):
        t = table[...]
        r = pltpu.roll(t, HEAD // 2, 1)
        low = lax.broadcasted_iota(jnp.int32, t.shape, 1) < HEAD // 2
        cos, sin = jnp.where(low, t, r), jnp.where(low, -r, t)
        for h in range(heads):
            v = wide(acc[:, h * HEAD : (h + 1) * HEAD].astype(q.dtype))
            put(h, (v * cos + pltpu.roll(v, HEAD // 2, 1) * sin).astype(q.dtype))

    def put_q(b):
        def put(h, v):
            q[h] = v
        turn(b, put)

    def put_k(b):
        def put(h, v):
            kc[h, rows_of(b * m, m), :] = v
        turn(b, put)

    def put_v(b):
        for h in range(heads):
            vt[h, 0:HEAD, pl.ds(pl.multiple_of(b * m, 128), m)] = acc[:, h * HEAD : (h + 1) * HEAD].T.astype(vt.dtype)

    e = HEAD**-0.5 * LOG2E
    group = min(heads, 4)

    def own(j):
        return pl.ds(pl.multiple_of(j * m, m), m)

    def score(j, h):
        return _dot(kc[h, own(j), :], q[h], 1, 1)

    def weigh(h, s, masked):
        if masked:
            ok = lax.broadcasted_iota(jnp.int32, s.shape, 0) <= lax.broadcasted_iota(jnp.int32, s.shape, 1)
            s = jnp.where(ok, s, HIDDEN)
        old = top[h]
        new = jnp.maximum(old, s.max(axis=0, keepdims=True))
        top[h] = new
        return jnp.exp2((s - new) * e).astype(vt.dtype), jnp.exp2((old - new) * e)

    def blend(j, h, w, k):
        mix[h] = mix[h] * k + _dot(vt[h, :, own(j)], w, 1, 0)

    def attend(j, hs, masked, pieces):
        n, r = len(pieces), len(hs)
        s, w = {}, {}

        def share(i):
            return range(r * i // n, r * (i + 1) // n) if 0 <= i < n else ()

        for i in range(n + 2):
            for h in share(i - 1):
                w[h] = weigh(hs[h], s.pop(h), masked)
            for h in share(i):
                s[h] = score(j, hs[h])
            for h in share(i - 2):
                blend(j, hs[h], *w.pop(h))
            if i < n:
                pieces[i]()

    def forget():
        top[...] = jnp.full(top.shape, NEG, jnp.float32)
        mix[...] = jnp.zeros(mix.shape, jnp.float32)

    def attention(b):
        attend(b, range(heads), True, [lambda: None] * 2)
        for h in range(heads):
            got = mix[h, 0:HEAD, :] * (1 / mix[h, HEAD : HEAD + 1, :])
            seen[:, h * HEAD : (h + 1) * HEAD] = got.T.astype(seen.dtype)

    def seen_copy(b):
        s = lax.rem(b, 2)
        return remote(seen, seenp.at[s], seen_send, seen_recv.at[s], mate)


    for k in range(NK):
        x_copy(0, k).start()
    barrier = pltpu.get_barrier_semaphore()
    friends = [mate] + [way(0, 0, stage)[1] for stage in range(3)]
    for friend in friends:
        pl.semaphore_signal(barrier, inc=1, device_id={"tp": friend}, device_id_type=pl.DeviceIdType.MESH)

    for h in range(heads):
        vt[h, HEAD:, :] = jnp.ones((ONES, sz.rows), vt.dtype)
    whole = wide(gain_in[...])
    for i in range(sz.wide // 128):
        gain[i * 128 // kt, :, i * 128 % kt : i * 128 % kt + 128] = whole[i : i + 1, :]

    def weights():
        for g in range(ahead):
            list(fetch(jnp.int32(g), g))[0]()
        table_copy(0).start()

    survey(0, weights)
    pl.semaphore_wait(barrier, len(friends))
    forget()

    def first(k, _):
        normed(k, 0, m // 2)
        share(k).start()
        x_copy(1, k).start()
        return 0

    lax.fori_loop(0, NK, first, 0)

    def rest(b):
        return remote(y.at[pl.ds(b * m, m), pl.ds(other, half)], y.at[pl.ds(b * m, m), pl.ds(other, half)], d_send.at[0, 0], d_recv.at[b], mate)

    pieces, now, held = _held(sz)
    early = -(-held // m)

    def hold(i):
        buffer, at, r, n, c, w = pieces[i]
        return local(y.at[pl.ds(r, n), pl.ds(c, w)], (send1, recv1, xb, vt, a, wb)[buffer].at[at], h_sem.at[i])

    def block(b, _):
        live = b < nb

        @pl.when(b == nb)
        def _():
            for i in range(early):
                rest(i).wait_recv()
            for i in range(now):
                hold(i).start()
            seen_copy(b - 1).wait_send()
            for t in range(NW):
                wx(t).wait_send()

        @pl.when(b == nb + 1)
        def _():
            for i in range(len(pieces)):
                hold(i).wait()

        @pl.when(live)
        def _():
            table_copy(b).wait()

        def actions(step, steps):
            for at in steps:
                for stage, p, back in _agenda(at):
                    @pl.when(step == at)
                    def _():
                        act(stage, p, b - back)

        def tick(phase, step):
            g = b * TILES + step
            s, k = lax.rem(g, sz.slots), lax.rem(step, NK)
            next_tile(g, phase, step)
            if phase == 0:
                @pl.when(g < NW)
                def _():
                    wx(g).start()

                share(k).wait()
            local(wq.at[pl.ds(0, kt)], wb.at[s], w_sem.at[s, 0]).wait()

            n = 4

            def piece(i):
                c = slice(i * inner // n, (i + 1) * inner // n)
                acc[:, c] += jnp.dot(a[k], wb[s, :, c], preferred_element_type=jnp.float32)

            pieces = [functools.partial(piece, i) for i in range(n)]

            def plain():
                for one in pieces:
                    one()

            if phase == 0:
                plain()
            else:
                i = (step - NK) * group
                j, h0 = lax.div(i, heads), lax.rem(i, heads)

                @pl.when(j < b)
                def _():
                    attend(j, [h0 + h for h in range(group)], False, pieces)

                @pl.when(j >= b)
                def _():
                    plain()

        for phase in range(3):
            def qkv_step(step, _, phase=phase):
                @pl.when(live)
                def _():
                    tick(phase, step)

                actions(step, range(phase * NK, (phase + 1) * NK))
                return 0

            acc[...] = jnp.zeros(acc.shape, jnp.float32)
            lax.fori_loop(phase * NK, (phase + 1) * NK, qkv_step, 0)
            if phase == 1:
                @pl.when(b == nb)
                def _():
                    for i in range(now, len(pieces)):
                        hold(i).start()

            @pl.when(live)
            def _(phase=phase):
                (put_q, put_k, put_v)[phase](b)

        @pl.when(live)
        def _():
            @pl.when(b > 0)
            def _():
                seen_copy(b - 1).wait_send()

            @pl.when(b + 1 < nb)
            def _():
                table_copy(b + 1).start()

            attention(b)
            seen_copy(b).start()
            forget()

            @pl.when(b + 1 < nb)
            def _():
                survey(b + 1)

        actions(MID, [MID])

        @pl.when(live)
        def _():
            seen_copy(b).wait_recv()

        def wo_step(step, _):
            @pl.when(live)
            def _():
                t = step - MID - 1
                g = b * TILES + 3 * NK + t
                s, ps = lax.rem(g, sz.slots), lax.rem(b, 2)
                next_tile(g, 3, 3 * NK + t)
                for i in range(2):
                    local(wo.at[:, pl.ds(0, wt)], wb.at[s, pl.ds(i * inner, inner), pl.ds(0, wt)], w_sem.at[s, i]).wait()
                for j in range(2):
                    n = t * 2 + j
                    p = jnp.where(n < 6, 0, jnp.where(n < 11, 1, 2))
                    bit = way(p, b, 0)[0]
                    go, stay = rows_of((1 - bit) * (m // 2), m // 2), rows_of(bit * (m // 2), m // 2)
                    here = jnp.concatenate([seen[go, :], seen[stay, :]], axis=0)
                    there = jnp.concatenate([seenp[ps, go, :], seenp[ps, stay, :]], axis=0)
                    c = slice(j * (wt // 2), (j + 1) * (wt // 2))
                    r = (jnp.dot(here, wb[s, 0:inner, c], preferred_element_type=jnp.float32)
                         + jnp.dot(there, wb[s, inner : 2 * inner, c], preferred_element_type=jnp.float32))
                    out = pl.ds(pl.multiple_of(n * (wt // 2), 128), wt // 2)
                    send1[:, out] = r[: m // 2].astype(send1.dtype)
                    keep[:, out] = r[m // 2 :]
                    normed(t, j * (m // 4), m // 4)

                @pl.when(b + 1 < nb)
                def _():
                    share(t).start()

                @pl.when(b + 2 < nb)
                def _():
                    x_copy(b + 2, t).start()

                for at, p in SENT.items():
                    @pl.when(step == at)
                    def _():
                        stage1(p, b).start()

            actions(step, range(MID + 1, STEPS))
            return 0

        lax.fori_loop(MID + 1, STEPS, wo_step, 0)
        return 0

    lax.fori_loop(0, nb + LAG, block, 0)
    for p in range(3):
        fin_sent(p, jnp.int32(nb - 1))
        pass_on(3, p, jnp.int32(nb - 1)).wait_send()
    for b in range(early, nb):
        rest(b).wait_recv()


def _collect(sz, y, send1, recv1, xb, vt, a, wb, out, ring, in_sem, out_sem, held_sem):
    pieces, _, first = _held(sz)
    slots, n = ring.shape[0], ring.shape[1]
    steps, ahead = (sz.rows - first) // n, slots // 2

    def held(i):
        buffer, at, r, k, c, w = pieces[i]
        return pltpu.make_async_copy((send1, recv1, xb, vt, a, wb)[buffer].at[at], out.at[pl.ds(r, k), pl.ds(c, w)], held_sem.at[i])

    def rows(i):
        return pl.ds(pl.multiple_of(first + i * n, n), n)

    def fetch(i):
        s = lax.rem(i, slots)
        return pltpu.make_async_copy(y.at[rows(i)], ring.at[s], in_sem.at[s])

    def store(i):
        s = lax.rem(i, slots)
        return pltpu.make_async_copy(ring.at[s], out.at[rows(i)], out_sem.at[s])

    for i in range(min(ahead, steps)):
        fetch(jnp.int32(i)).start()
    for i in range(len(pieces)):
        held(i).start()

    def one(i, _):
        fetch(i).wait()
        store(i).start()

        @pl.when(i + ahead < steps)
        def _():
            @pl.when(i + ahead >= slots)
            def _():
                store(i + ahead - slots).wait()

            fetch(i + ahead).start()
        return 0

    def end(i, _):
        store(i).wait()
        return 0

    lax.fori_loop(0, steps, one, 0)
    lax.fori_loop(max(steps - slots, 0), steps, end, 0)
    for i in range(len(pieces)):
        held(i).wait()


def _angles(rows):
    half = HEAD // 2
    step = np.power(np.float32(THETA), -np.arange(half, dtype=np.float32) / np.float32(half)).astype(np.float32)
    angle = (np.arange(rows, dtype=np.float32)[:, None] * step).astype(np.float64)
    return np.concatenate([np.cos(angle), np.sin(angle)], -1).astype(np.float32)


def layer(sz, x, gain, wq, wk, wv, wo):
    low, f32 = x.dtype, jnp.float32
    m, inner, half = sz.m, sz.inner, sz.half
    vmem, dma = pltpu.VMEM, pltpu.SemaphoreType.DMA
    pieces, _, held = _held(sz)
    kept = [
        vmem((m // 2, half), low),
        vmem((m // 2, half), low),
        vmem((NK, m // 2, sz.kt), low),
        vmem((sz.heads, HEAD + ONES, sz.rows), low),
        vmem((NK, m, sz.kt), low),
        vmem((sz.slots, sz.kt, inner), low),
    ]
    scratch = [
        vmem((NK, 1, sz.kt), f32),
        vmem((m // 2, 128), f32),
        vmem((m, HEAD), f32),
        vmem((sz.heads, sz.rows, HEAD), low),
        vmem((sz.heads, m, HEAD), low),
        vmem((m, inner), low),
        vmem((2, m, inner), low),
        vmem((m, inner), f32),
        vmem((sz.heads, HEAD + ONES, m), f32),
        vmem((sz.heads, 1, m), f32),
        vmem((m // 2, half), f32),
        vmem((m // 4, half), low),
        vmem((m // 4, half), low),
        vmem((m // 8, half), low),
        vmem((2, m // 8, half), low),
        vmem((m // 8, half), low),
        vmem((m // 8, half), low),
        dma((sz.slots, 2)), dma((NK,)), dma((NK,)), dma((NK,)), dma, dma((3,)), dma((NW,)), dma((NW,)), dma, dma((2,)),
        dma((3, 3)), dma((3, 2, 3)), dma((6, 3)), dma((6, 2, 3)), dma((3,)), dma((4, 3)), dma((sz.blocks,)), dma((len(pieces),)),
    ]
    hbm, here = pl.BlockSpec(memory_space=pl.ANY), pl.BlockSpec(memory_space=pltpu.VMEM)
    flops = 2 * sz.rows * sz.wide * 4 * inner + 2 * sz.rows * sz.rows * 2 * inner
    y, _, *kept = pl.pallas_call(
        functools.partial(_kernel, sz),
        out_shape=[jax.ShapeDtypeStruct(x.shape, low), jax.ShapeDtypeStruct((inner, half), low), *kept],
        in_specs=[hbm] * 6 + [here],
        out_specs=[hbm] * 2 + [here] * 6,
        scratch_shapes=scratch,
        compiler_params=pltpu.CompilerParams(collective_id=0, has_side_effects=True, vmem_limit_bytes=21 * 2**20),
        cost_estimate=pl.CostEstimate(flops=flops, bytes_accessed=4 * sz.blocks * inner * sz.wide * 2,
                                      transcendentals=sz.rows * sz.rows * sz.heads),
        name="decoder_attention",
    )(x, wq, wk, wv, wo, jnp.asarray(_angles(sz.rows)), gain.reshape(sz.wide // 128, 128))
    kept = [pltpu.with_memory_space_constraint(v, pltpu.MemorySpace.VMEM) for v in kept]
    ring, n = 8, min(64, sz.rows - held)
    return pl.pallas_call(
        functools.partial(_collect, sz),
        out_shape=jax.ShapeDtypeStruct(x.shape, low),
        in_specs=[hbm] * 7,
        out_specs=hbm,
        scratch_shapes=[vmem((ring, n, sz.wide), low), dma((ring,)), dma((ring,)), dma((len(pieces),))],
        compiler_params=pltpu.CompilerParams(vmem_limit_bytes=18 * 2**20),
        cost_estimate=pl.CostEstimate(flops=0, bytes_accessed=3 * sz.rows * sz.wide, transcendentals=0),
        name="collect",
    )(y, *kept)


def solution(mesh):
    def step(x, gain, wq, wk, wv, wo):
        sz = Sizes(rows=x.shape[0], wide=x.shape[1], heads=wq.shape[1] // HEAD)
        return layer(sz, x, gain, wq, wk, wv, wo)

    tokens, columns = P("dp", None), P(None, "tp")
    return jax.shard_map(
        step,
        mesh=mesh,
        in_specs=(tokens, P(None), columns, columns, columns, P("tp", None)),
        out_specs=tokens,
        check_vma=False,
    )
```

```python
import functools
from typing import NamedTuple

import jax
import jax.numpy as jnp
import numpy as np
from jax import lax
from jax.experimental import pallas as pl
from jax.experimental.pallas import tpu as pltpu
from jax.sharding import PartitionSpec as P

HEAD = 128
THETA = 10000
EPS = 1e-6
NEG = -1e30
HIDDEN = 2 * NEG
LOG2E = 1.4426950408889634
ONES = 16
NK = 8
NW = 8
TILES = 3 * NK + NW
MID = 3 * NK
STEPS = MID + 1 + NW


class Sizes(NamedTuple):
    rows: int
    wide: int
    heads: int
    m: int = 256
    slots: int = 5

    @property
    def blocks(self):
        return self.rows // self.m

    @property
    def inner(self):
        return self.heads * HEAD

    @property
    def half(self):
        return self.wide // 2

    @property
    def kt(self):
        return self.wide // NK

    @property
    def wt(self):
        return self.half // NW

    @property
    def parts(self):
        u = self.wt // 2
        return (0, 6 * u), (6 * u, 5 * u), (11 * u, 5 * u)


WHEN = {
    "add1": (8, 9, 11),
    "add2": (17, 16, 18),
    "add3": (24, 21, 23),
    "gather2": (36, 33, 27),
    "gather3": (46, 50, 41),
    "last": (63, 57, 54),
}
HALVES = ((0, 3), (3, 3), (6, 3), (9, 2), (11, 3), (14, 2))
SENT = {MID + 2: 0, MID + 4: 2, MID + 5: 3, MID + 6: 4, MID + 7: 1, MID + 8: 5}
LAG = max(max(w) for w in WHEN.values()) // STEPS + 1


def _held(sz):
    rows = sz.kt // 2
    pieces = [(5, (i // 2, slice(i % 2 * rows, (i % 2 + 1) * rows)), 0, rows, i * sz.inner, sz.inner) for i in range(2 * sz.slots)]
    tiles = [(r, c) for r in range(0, rows, sz.m) for c in range(2 * sz.slots * sz.inner, sz.wide, sz.kt)]
    pieces += [(4, (i,), r, sz.m, c, sz.kt) for i, (r, c) in enumerate(tiles[:NK])]
    n = sz.m // 2
    pieces += [(2, (2 * i + j,), r + j * n, n, c, sz.kt) for i, (r, c) in enumerate(tiles[NK:]) for j in range(2)]
    w = sz.wide // sz.heads
    if w <= sz.rows:
        pieces += [(3, (h, slice(0, HEAD), slice(0, w)), rows, HEAD, h * w, w) for h in range(sz.heads)]
        rows += HEAD
    now = len(pieces)
    pieces += [(i, (), rows, n, i * sz.half, sz.half) for i in range(2)]
    return pieces, now, rows + n


def _agenda(step):
    return [(stage, p, 1 + w[p] // STEPS) for stage, w in WHEN.items() for p in range(3) if w[p] % STEPS == step]


def _dot(a, b, ca, cb):
    return lax.dot_general(a, b, (((ca,), (cb,)), ((), ())), preferred_element_type=jnp.float32)


def _kernel(sz, x, wq, wk, wv, wo, angles, gain_in, y, wpart, send1, recv1, xb, vt, a, wb,
            gain, ssq, table, kc, q, seen, seenp, acc, mix, top, keep, send2, recv2, send3, recv3, fin, xr,
            w_sem, x_sem, n_send, n_recv, t_sem, xr_sem, wx_send, wx_recv, seen_send, seen_recv, s1_send, s1_recv, s_sem, r_sem, g_send, g_recv, own_sem, d_send, d_recv, h_sem):
    m, nb, heads, inner, half, kt, wt = sz.m, sz.blocks, sz.heads, sz.inner, sz.half, sz.kt, sz.wt
    total = nb * TILES
    me = lax.axis_index("tp")
    core = lax.rem(me, 2)
    mate = me + 1 - 2 * core
    mine, other = pl.multiple_of(core * half, 128), pl.multiple_of((1 - core) * half, 128)

    def local(src, dst, sem):
        return pltpu.make_async_copy(src, dst, sem)

    def remote(src, dst, send, recv, to):
        return pltpu.make_async_remote_copy(src_ref=src, dst_ref=dst, send_sem=send, recv_sem=recv, device_id={"tp": to},
                                            device_id_type=pl.DeviceIdType.MESH)

    def rows_of(i, n):
        return pl.ds(pl.multiple_of(i, 16), n)


    def x_copy(b, k):
        at = rows_of(b * m + core * (m // 2), m // 2)
        return local(x.at[at, pl.ds(pl.multiple_of(k * kt, 128), kt)], xb.at[k], x_sem.at[k])

    def share(k):
        part = a.at[k, rows_of(core * (m // 2), m // 2)]
        return remote(part, part, n_send.at[k], n_recv.at[k], mate)

    def wx(t):
        c = pl.multiple_of(t * wt, 128)
        return remote(wo.at[:, pl.ds(pl.multiple_of(other + c, 128), wt)], wpart.at[:, pl.ds(c, wt)], wx_send.at[t], wx_recv.at[t], mate)

    def tile_at(t):
        return t + jnp.where((t >= 2) & (t < 6), 1, 0) - jnp.where(t == 6, 4, 0)

    def fetch(g, j):
        s = lax.rem(g, sz.slots)

        def weight(w, k):
            local(w.at[rows_of(k * kt, kt)], wb.at[s], w_sem.at[s, 0]).start()

        def out(t):
            c = pl.multiple_of(tile_at(t) * wt, 128)
            local(wo.at[:, pl.ds(pl.multiple_of(mine + c, 128), wt)], wb.at[s, pl.ds(0, inner), pl.ds(0, wt)], w_sem.at[s, 0]).start()
            local(wpart.at[:, pl.ds(c, wt)], wb.at[s, pl.ds(inner, inner), pl.ds(0, wt)], w_sem.at[s, 1]).start()

        for i, w in enumerate((wq, wk, wv)):
            yield lambda w=w, i=i: weight(w, j - i * NK)
        yield lambda: out(j - 3 * NK)

    ahead = sz.slots - 1

    def next_tile(g, phase, step):
        last = (phase + 1) * NK - ahead
        here, there = list(fetch(g + ahead, step + ahead)), list(fetch(g + ahead, step + ahead - (TILES if phase == 3 else 0)))

        def traded():
            @pl.when(g + ahead < TILES)
            def _():
                wx(tile_at(g + ahead - 3 * NK)).wait_recv()

        @pl.when(step < last)
        def _():
            if phase == 3:
                traded()
            here[phase]()

        @pl.when((step >= last) & (g + ahead < total))
        def _():
            if phase == 2:
                traded()
            there[(phase + 1) % 4]()

    def table_copy(b):
        return local(angles.at[rows_of(b * m, m)], table, t_sem)


    def way(p, b, stage):
        axis = lax.rem(p + stage + b, 3)
        mask = 8 - 5 * axis + axis * axis
        bit = lax.rem(lax.div(me, mask), 2)
        return bit, me + mask * (1 - 2 * bit)

    def ways(p, b):
        return [way(p, b, stage) for stage in range(3)]

    def place(p, b, off, n):
        return rows_of(b * m + off, n), pl.ds(pl.multiple_of(mine + sz.parts[p][0], 128), sz.parts[p][1])

    def cols(p):
        return pl.ds(*sz.parts[p])

    def strips(p, body):
        c0, n = sz.parts[p]
        step = sz.wt // 2

        def one(i, _):
            body(pl.ds(pl.multiple_of(c0 + i * step, 128), step))
            return 0

        lax.fori_loop(0, n // step, one, 0)

    def wide(v):
        return v.astype(jnp.float32)

    def stage1(half_part, b):
        first, n = HALVES[half_part]
        c = pl.ds(first * (wt // 2), n * (wt // 2))
        return remote(send1.at[:, c], recv1.at[:, c], s1_send.at[half_part], s1_recv.at[lax.rem(b, 2), half_part],
                      ways(half_part // 2, b)[0][1])

    def stage2(p, b):
        return remote(send2.at[:, cols(p)], recv2.at[:, cols(p)], s_sem.at[1, p], r_sem.at[1, lax.rem(b, 2), p],
                      ways(p, b)[1][1])

    def stage3(p, b):
        return remote(send3.at[:, cols(p)], recv3.at[lax.rem(b, 2), :, cols(p)], s_sem.at[2, p], r_sem.at[2, lax.rem(b, 2), p],
                      ways(p, b)[2][1])

    def offsets(p, b):
        (b1, _), (b2, _), (b3, _) = ways(p, b)
        return b1 * (m // 2), b1 * (m // 2) + b2 * (m // 4), b1 * (m // 2) + b2 * (m // 4) + b3 * (m // 8)

    def xr_copy(p, b):
        return local(x.at[place(p, b, offsets(p, b)[2], m // 8)], xr.at[:, cols(p)], xr_sem.at[p])

    def own_copy(p, b):
        return local(fin.at[:, cols(p)], y.at[place(p, b, offsets(p, b)[2], m // 8)], own_sem.at[p])

    def gather(kind, p, b):
        w, o = ways(p, b), offsets(p, b)
        n, axis = m // 8, (2, 1, 0, 1, 0, 0)[kind]
        if kind < 3:
            at, src = place(p, b, o[2], n), fin.at[:, cols(p)]
        else:
            if kind < 5:
                at = place(p, b, o[1] + (1 - w[2][0]) * n, n)
            else:
                at = place(p, b, o[0] + (1 - w[1][0]) * 2 * n, 2 * n)
            src = y.at[at]
        return remote(src, y.at[at], g_send.at[kind, p], g_recv.at[kind, lax.rem(b, 2), p], w[axis][1])

    def pass_on(kind, p, b):
        o = offsets(p, b)
        w = ways(p, b)
        if kind == 0:
            at, src = place(p, b, o[2], m // 8), fin.at[:, cols(p)]
        else:
            if kind < 3:
                n = m // 8 << (kind - 1)
                off = o[2 - kind] + (1 - w[3 - kind][0]) * n
            else:
                n = m // 4
                bit = w[1][0]
                off = (1 - w[0][0]) * (m // 2) + (bit if kind == 3 else 1 - bit) * n
            at = place(p, b, off, n)
            src = y.at[at]
        return remote(src, y.at[at], d_send.at[kind, p], d_recv.at[b], mate)

    def add1(p, b):
        w = ways(p, b)
        stage1(2 * p, b).wait()
        stage1(2 * p + 1, b).wait()
        h = m // 4
        go, stay = rows_of((1 - w[1][0]) * h, h), rows_of(w[1][0] * h, h)

        def body(c):
            send2[:, c] = (keep[go, c] + wide(recv1[go, c])).astype(send2.dtype)
            keep[stay, c] = keep[stay, c] + wide(recv1[stay, c])

        strips(p, body)
        stage2(p, b).start()

    def add2(p, b):
        w = ways(p, b)
        xr_copy(p, b).start()
        stage2(p, b).wait()
        h = m // 8
        base, go, stay = w[1][0] * (m // 4), (1 - w[2][0]) * h, w[2][0] * h

        def body(c):
            send3[:, c] = (keep[rows_of(base + go, h), c] + wide(recv2[rows_of(go, h), c])).astype(send3.dtype)
            keep[rows_of(base + stay, h), c] = keep[rows_of(base + stay, h), c] + wide(recv2[rows_of(stay, h), c])

        strips(p, body)
        stage3(p, b).start()

    def fin_sent(p, b):
        for kind in range(3):
            gather(kind, p, b).wait_send()
        own_copy(p, b).wait()
        pass_on(0, p, b).wait_send()

    def add3(p, b):
        s, w = lax.rem(b, 2), ways(p, b)

        @pl.when(b > 0)
        def _():
            fin_sent(p, b - 1)

        xr_copy(p, b).wait()
        stage3(p, b).wait()
        h = m // 8
        at = rows_of(w[1][0] * (m // 4) + w[2][0] * h, h)

        def body(c):
            fin[:, c] = (wide(xr[:, c]) + (keep[at, c] + wide(recv3[s, :, c]))).astype(fin.dtype)

        strips(p, body)
        for kind in range(3):
            gather(kind, p, b).start()
        own_copy(p, b).start()
        pass_on(0, p, b).start()

    def gather2(p, b):
        gather(0, p, b).wait_recv()
        for kind in (3, 4):
            gather(kind, p, b).start()
        pass_on(1, p, b).start()

    def gather3(p, b):
        gather(1, p, b).wait_recv()
        gather(3, p, b).wait_recv()
        gather(5, p, b).start()
        pass_on(2, p, b).start()
        gather(3, p, b).wait_send()
        pass_on(1, p, b).wait_send()

    def last(p, b):
        @pl.when(b > 0)
        def _():
            for kind in (3, 4):
                pass_on(kind, p, b - 1).wait_send()

        for kind in (2, 4):
            gather(kind, p, b).wait_recv()
        pass_on(3, p, b).start()
        gather(5, p, b).wait_recv()
        pass_on(4, p, b).start()
        for kind in (4, 5):
            gather(kind, p, b).wait_send()
        pass_on(2, p, b).wait_send()

    stages = {"add1": add1, "add2": add2, "add3": add3, "gather2": gather2, "gather3": gather3, "last": last}

    def act(stage, p, b):
        @pl.when((b >= 0) & (b < nb))
        def _():
            stages[stage](p, b)


    def survey(b, meanwhile=None):
        ssq[...] = jnp.zeros(ssq.shape, jnp.float32)

        def one(k, _):
            x_copy(b, k).wait()
            total = ssq[...]
            for c in range(0, kt, 128):
                v = wide(xb[k, :, c : c + 128])
                total = total + v * v
            ssq[...] = total
            return 0

        if meanwhile is None:
            lax.fori_loop(0, NK, one, 0)
        else:
            lax.fori_loop(0, NK // 2, one, 0)
            meanwhile()
            lax.fori_loop(NK // 2, NK, one, 0)
        total = jnp.sum(ssq[...], axis=1, keepdims=True)
        ssq[...] = jnp.broadcast_to(lax.rsqrt(total * (1 / sz.wide) + EPS), ssq.shape)

    def normed(k, first, n):
        at, to = slice(first, first + n), rows_of(core * (m // 2) + first, n)
        for c in range(0, kt, 128):
            v = wide(xb[k, at, c : c + 128]) * ssq[at, :] * gain[k, :, c : c + 128]
            a[k, to, c : c + 128] = v.astype(a.dtype)

    def turn(b, put):
        t = table[...]
        r = pltpu.roll(t, HEAD // 2, 1)
        low = lax.broadcasted_iota(jnp.int32, t.shape, 1) < HEAD // 2
        cos, sin = jnp.where(low, t, r), jnp.where(low, -r, t)
        for h in range(heads):
            v = wide(acc[:, h * HEAD : (h + 1) * HEAD].astype(q.dtype))
            put(h, (v * cos + pltpu.roll(v, HEAD // 2, 1) * sin).astype(q.dtype))

    def put_q(b):
        def put(h, v):
            q[h] = v
        turn(b, put)

    def put_k(b):
        def put(h, v):
            kc[h, rows_of(b * m, m), :] = v
        turn(b, put)

    def put_v(b):
        for h in range(heads):
            vt[h, 0:HEAD, pl.ds(pl.multiple_of(b * m, 128), m)] = acc[:, h * HEAD : (h + 1) * HEAD].T.astype(vt.dtype)

    e = HEAD**-0.5 * LOG2E
    group = min(heads, 4)

    def own(j):
        return pl.ds(pl.multiple_of(j * m, m), m)

    def score(j, h):
        return _dot(kc[h, own(j), :], q[h], 1, 1)

    def weigh(h, s, masked):
        if masked:
            ok = lax.broadcasted_iota(jnp.int32, s.shape, 0) <= lax.broadcasted_iota(jnp.int32, s.shape, 1)
            s = jnp.where(ok, s, HIDDEN)
        old = top[h]
        new = jnp.maximum(old, s.max(axis=0, keepdims=True))
        top[h] = new
        return jnp.exp2((s - new) * e).astype(vt.dtype), jnp.exp2((old - new) * e)

    def blend(j, h, w, k):
        mix[h] = mix[h] * k + _dot(vt[h, :, own(j)], w, 1, 0)

    def attend(j, hs, masked, pieces):
        n, r = len(pieces), len(hs)
        s, w = {}, {}

        def share(i):
            return range(r * i // n, r * (i + 1) // n) if 0 <= i < n else ()

        for i in range(n + 2):
            for h in share(i - 1):
                w[h] = weigh(hs[h], s.pop(h), masked)
            for h in share(i):
                s[h] = score(j, hs[h])
            for h in share(i - 2):
                blend(j, hs[h], *w.pop(h))
            if i < n:
                pieces[i]()

    def forget():
        top[...] = jnp.full(top.shape, NEG, jnp.float32)
        mix[...] = jnp.zeros(mix.shape, jnp.float32)

    def attention(b):
        attend(b, range(heads), True, [lambda: None] * 2)
        for h in range(heads):
            got = mix[h, 0:HEAD, :] * (1 / mix[h, HEAD : HEAD + 1, :])
            seen[:, h * HEAD : (h + 1) * HEAD] = got.T.astype(seen.dtype)

    def seen_copy(b):
        s = lax.rem(b, 2)
        return remote(seen, seenp.at[s], seen_send, seen_recv.at[s], mate)


    for k in range(NK):
        x_copy(0, k).start()
    barrier = pltpu.get_barrier_semaphore()
    friends = [mate] + [way(0, 0, stage)[1] for stage in range(3)]
    for friend in friends:
        pl.semaphore_signal(barrier, inc=1, device_id={"tp": friend}, device_id_type=pl.DeviceIdType.MESH)

    for h in range(heads):
        vt[h, HEAD:, :] = jnp.ones((ONES, sz.rows), vt.dtype)
    whole = wide(gain_in[...])
    for i in range(sz.wide // 128):
        gain[i * 128 // kt, :, i * 128 % kt : i * 128 % kt + 128] = whole[i : i + 1, :]

    def weights():
        for g in range(ahead):
            list(fetch(jnp.int32(g), g))[0]()
        table_copy(0).start()

    survey(0, weights)
    pl.semaphore_wait(barrier, len(friends))
    forget()

    def first(k, _):
        normed(k, 0, m // 2)
        share(k).start()
        x_copy(1, k).start()
        return 0

    lax.fori_loop(0, NK, first, 0)

    def rest(b):
        return remote(y.at[pl.ds(b * m, m), pl.ds(other, half)], y.at[pl.ds(b * m, m), pl.ds(other, half)], d_send.at[0, 0], d_recv.at[b], mate)

    pieces, now, held = _held(sz)
    early = -(-held // m)

    def hold(i):
        buffer, at, r, n, c, w = pieces[i]
        return local(y.at[pl.ds(r, n), pl.ds(c, w)], (send1, recv1, xb, vt, a, wb)[buffer].at[at], h_sem.at[i])

    def block(b, _):
        live = b < nb

        @pl.when(b == nb)
        def _():
            for i in range(early):
                rest(i).wait_recv()
            for i in range(now):
                hold(i).start()
            seen_copy(b - 1).wait_send()
            for t in range(NW):
                wx(t).wait_send()

        @pl.when(b == nb + 1)
        def _():
            for i in range(len(pieces)):
                hold(i).wait()

        @pl.when(live)
        def _():
            table_copy(b).wait()

        def actions(step, steps):
            for at in steps:
                for stage, p, back in _agenda(at):
                    @pl.when(step == at)
                    def _():
                        act(stage, p, b - back)

        def tick(phase, step):
            g = b * TILES + step
            s, k = lax.rem(g, sz.slots), lax.rem(step, NK)
            next_tile(g, phase, step)
            if phase == 0:
                @pl.when(g < NW)
                def _():
                    wx(g).start()

                share(k).wait()
            local(wq.at[pl.ds(0, kt)], wb.at[s], w_sem.at[s, 0]).wait()

            n = 4

            def piece(i):
                c = slice(i * inner // n, (i + 1) * inner // n)
                acc[:, c] += jnp.dot(a[k], wb[s, :, c], preferred_element_type=jnp.float32)

            pieces = [functools.partial(piece, i) for i in range(n)]

            def plain():
                for one in pieces:
                    one()

            if phase == 0:
                plain()
            else:
                i = (step - NK) * group
                j, h0 = lax.div(i, heads), lax.rem(i, heads)

                @pl.when(j < b)
                def _():
                    attend(j, [h0 + h for h in range(group)], False, pieces)

                @pl.when(j >= b)
                def _():
                    plain()

        for phase in range(3):
            def qkv_step(step, _, phase=phase):
                @pl.when(live)
                def _():
                    tick(phase, step)

                actions(step, range(phase * NK, (phase + 1) * NK))
                return 0

            acc[...] = jnp.zeros(acc.shape, jnp.float32)
            lax.fori_loop(phase * NK, (phase + 1) * NK, qkv_step, 0)
            if phase == 1:
                @pl.when(b == nb)
                def _():
                    for i in range(now, len(pieces)):
                        hold(i).start()

            @pl.when(live)
            def _(phase=phase):
                (put_q, put_k, put_v)[phase](b)

        @pl.when(live)
        def _():
            @pl.when(b > 0)
            def _():
                seen_copy(b - 1).wait_send()

            @pl.when(b + 1 < nb)
            def _():
                table_copy(b + 1).start()

            attention(b)
            seen_copy(b).start()
            forget()

            @pl.when(b + 1 < nb)
            def _():
                survey(b + 1)

        actions(MID, [MID])

        @pl.when(live)
        def _():
            seen_copy(b).wait_recv()

        def wo_step(step, _):
            @pl.when(live)
            def _():
                t = step - MID - 1
                g = b * TILES + 3 * NK + t
                s, ps = lax.rem(g, sz.slots), lax.rem(b, 2)
                next_tile(g, 3, 3 * NK + t)
                for i in range(2):
                    local(wo.at[:, pl.ds(0, wt)], wb.at[s, pl.ds(i * inner, inner), pl.ds(0, wt)], w_sem.at[s, i]).wait()
                for j in range(2):
                    n = tile_at(t) * 2 + j
                    p = jnp.where(n < 6, 0, jnp.where(n < 11, 1, 2))
                    bit = way(p, b, 0)[0]
                    go, stay = rows_of((1 - bit) * (m // 2), m // 2), rows_of(bit * (m // 2), m // 2)
                    here = jnp.concatenate([seen[go, :], seen[stay, :]], axis=0)
                    there = jnp.concatenate([seenp[ps, go, :], seenp[ps, stay, :]], axis=0)
                    c = slice(j * (wt // 2), (j + 1) * (wt // 2))
                    r = (jnp.dot(here, wb[s, 0:inner, c], preferred_element_type=jnp.float32)
                         + jnp.dot(there, wb[s, inner : 2 * inner, c], preferred_element_type=jnp.float32))
                    out = pl.ds(pl.multiple_of(n * (wt // 2), 128), wt // 2)
                    send1[:, out] = r[: m // 2].astype(send1.dtype)
                    keep[:, out] = r[m // 2 :]
                    normed(t, j * (m // 4), m // 4)

                @pl.when(b + 1 < nb)
                def _():
                    share(t).start()

                @pl.when(b + 2 < nb)
                def _():
                    x_copy(b + 2, t).start()

                for at, p in SENT.items():
                    @pl.when(step == at)
                    def _():
                        stage1(p, b).start()

            actions(step, range(MID + 1, STEPS))
            return 0

        lax.fori_loop(MID + 1, STEPS, wo_step, 0)
        return 0

    lax.fori_loop(0, nb + LAG, block, 0)
    for p in range(3):
        fin_sent(p, jnp.int32(nb - 1))
        for kind in (3, 4):
            pass_on(kind, p, jnp.int32(nb - 1)).wait_send()
    for b in range(early, nb):
        rest(b).wait_recv()


def _collect(sz, y, send1, recv1, xb, vt, a, wb, out, ring, in_sem, out_sem, held_sem):
    pieces, _, first = _held(sz)
    slots, n = ring.shape[0], ring.shape[1]
    steps, ahead = (sz.rows - first) // n, slots // 2

    def held(i):
        buffer, at, r, k, c, w = pieces[i]
        return pltpu.make_async_copy((send1, recv1, xb, vt, a, wb)[buffer].at[at], out.at[pl.ds(r, k), pl.ds(c, w)], held_sem.at[i])

    def rows(i):
        return pl.ds(pl.multiple_of(first + i * n, n), n)

    def fetch(i):
        s = lax.rem(i, slots)
        return pltpu.make_async_copy(y.at[rows(i)], ring.at[s], in_sem.at[s])

    def store(i):
        s = lax.rem(i, slots)
        return pltpu.make_async_copy(ring.at[s], out.at[rows(i)], out_sem.at[s])

    for i in range(min(ahead, steps)):
        fetch(jnp.int32(i)).start()
    for i in range(len(pieces)):
        held(i).start()

    def one(i, _):
        fetch(i).wait()
        store(i).start()

        @pl.when(i + ahead < steps)
        def _():
            @pl.when(i + ahead >= slots)
            def _():
                store(i + ahead - slots).wait()

            fetch(i + ahead).start()
        return 0

    def end(i, _):
        store(i).wait()
        return 0

    lax.fori_loop(0, steps, one, 0)
    lax.fori_loop(max(steps - slots, 0), steps, end, 0)
    for i in range(len(pieces)):
        held(i).wait()


def _angles(rows):
    half = HEAD // 2
    step = np.power(np.float32(THETA), -np.arange(half, dtype=np.float32) / np.float32(half)).astype(np.float32)
    angle = (np.arange(rows, dtype=np.float32)[:, None] * step).astype(np.float64)
    return np.concatenate([np.cos(angle), np.sin(angle)], -1).astype(np.float32)


def layer(sz, x, gain, wq, wk, wv, wo):
    low, f32 = x.dtype, jnp.float32
    m, inner, half = sz.m, sz.inner, sz.half
    vmem, dma = pltpu.VMEM, pltpu.SemaphoreType.DMA
    pieces, _, held = _held(sz)
    kept = [
        vmem((m // 2, half), low),
        vmem((m // 2, half), low),
        vmem((NK, m // 2, sz.kt), low),
        vmem((sz.heads, HEAD + ONES, sz.rows), low),
        vmem((NK, m, sz.kt), low),
        vmem((sz.slots, sz.kt, inner), low),
    ]
    scratch = [
        vmem((NK, 1, sz.kt), f32),
        vmem((m // 2, 128), f32),
        vmem((m, HEAD), f32),
        vmem((sz.heads, sz.rows, HEAD), low),
        vmem((sz.heads, m, HEAD), low),
        vmem((m, inner), low),
        vmem((2, m, inner), low),
        vmem((m, inner), f32),
        vmem((sz.heads, HEAD + ONES, m), f32),
        vmem((sz.heads, 1, m), f32),
        vmem((m // 2, half), f32),
        vmem((m // 4, half), low),
        vmem((m // 4, half), low),
        vmem((m // 8, half), low),
        vmem((2, m // 8, half), low),
        vmem((m // 8, half), low),
        vmem((m // 8, half), low),
        dma((sz.slots, 2)), dma((NK,)), dma((NK,)), dma((NK,)), dma, dma((3,)), dma((NW,)), dma((NW,)), dma, dma((2,)),
        dma((6,)), dma((2, 6)), dma((3, 3)), dma((3, 2, 3)), dma((6, 3)), dma((6, 2, 3)), dma((3,)), dma((5, 3)), dma((sz.blocks,)), dma((len(pieces),)),
    ]
    hbm, here = pl.BlockSpec(memory_space=pl.ANY), pl.BlockSpec(memory_space=pltpu.VMEM)
    flops = 2 * sz.rows * sz.wide * 4 * inner + 2 * sz.rows * sz.rows * 2 * inner
    y, _, *kept = pl.pallas_call(
        functools.partial(_kernel, sz),
        out_shape=[jax.ShapeDtypeStruct(x.shape, low), jax.ShapeDtypeStruct((inner, half), low), *kept],
        in_specs=[hbm] * 6 + [here],
        out_specs=[hbm] * 2 + [here] * 6,
        scratch_shapes=scratch,
        compiler_params=pltpu.CompilerParams(collective_id=0, has_side_effects=True, vmem_limit_bytes=21 * 2**20),
        cost_estimate=pl.CostEstimate(flops=flops, bytes_accessed=4 * sz.blocks * inner * sz.wide * 2,
                                      transcendentals=sz.rows * sz.rows * sz.heads),
        name="decoder_attention",
    )(x, wq, wk, wv, wo, jnp.asarray(_angles(sz.rows)), gain.reshape(sz.wide // 128, 128))
    kept = [pltpu.with_memory_space_constraint(v, pltpu.MemorySpace.VMEM) for v in kept]
    ring, n = 8, min(64, sz.rows - held)
    return pl.pallas_call(
        functools.partial(_collect, sz),
        out_shape=jax.ShapeDtypeStruct(x.shape, low),
        in_specs=[hbm] * 7,
        out_specs=hbm,
        scratch_shapes=[vmem((ring, n, sz.wide), low), dma((ring,)), dma((ring,)), dma((len(pieces),))],
        compiler_params=pltpu.CompilerParams(vmem_limit_bytes=18 * 2**20),
        cost_estimate=pl.CostEstimate(flops=0, bytes_accessed=3 * sz.rows * sz.wide, transcendentals=0),
        name="collect",
    )(y, *kept)


def solution(mesh):
    def step(x, gain, wq, wk, wv, wo):
        sz = Sizes(rows=x.shape[0], wide=x.shape[1], heads=wq.shape[1] // HEAD)
        return layer(sz, x, gain, wq, wk, wv, wo)

    tokens, columns = P("dp", None), P(None, "tp")
    return jax.shard_map(
        step,
        mesh=mesh,
        in_specs=(tokens, P(None), columns, columns, columns, P("tp", None)),
        out_specs=tokens,
        check_vma=False,
    )
```
